128 devices in a mesh: row: 32 (over x, z, core), col: 4 (over y).
Axes of the slice: x: 4, y: 4, z: 4, core: 2. Of those that a mesh axis runs over, the one named last changes fastest.
Arguments:
- hub_seeds: bfloat16 [768, 64, 128], P('row'), may hold values from -6 to 6
- tile_blocks: bfloat16 [98304, 128, 128], P(('row', 'col')), may hold values from -8 to 8
- tile_rows: int32 [98304], P(('row', 'col')), may hold values from 0 to 511, as said below
- tile_cols: int32 [98304], P(('row', 'col')), may hold values from 0 to 511, as said below
- tile_count: int32 [128], P(('row', 'col')), may hold values from 192 to 768, as said below
- row_blocks: int32 [32], replicated, may hold values from 8 to 24, as said below
Outputs:
- authority: bfloat16 [512, 64, 128], P(('row', 'col'))
- hub_scores: bfloat16 [768, 64, 128], P('row')
The draws below stay inside these ranges and needn't reach their ends.
Inputs may be any that keep to these rules, and one draw needn't show every extreme that they name: Row range r covers row blocks starts[r] to starts[r] + row_blocks[r] - 1, the ranges in order and together all 512 blocks; the longest range has exactly 24 blocks in every draw. `tile_rows`: every tile of a device lies in the row range of the device's row index; no pair of row block and column block repeats within a device. `tile_cols`: A device with column index c holds only column blocks b with (b // 4) % 4 == c. The live tiles of a device are its first tile_count slots; some device has all 768 slots live in every draw.
All inputs are finite; a program needn't handle non-finite values.
Results may differ from the reference program's by a relative error of at most 0.02.
Values may be sent and summed in bfloat16 or wider, within the bound.
No kernel may reach another device: no remote copies, remote signals or barrier semaphores. Data moves between devices by JAX's collectives and lax.ppermute only.
A program may use at most 192 MiB of HBM per device.

```python
import jax
import jax.numpy as jnp
from jax import lax

K = 64
TB = 128
ITERS = 2
RB_DEV = 16
ROWDEV = 32
COLDEV = 4
NB = 512
HOSTS = 65536
LMAX = 24
COLUMN_BLOCKS_SET = 128
GROUP = 4
TILE_DEV = 768


def tile_layout(key):
    base_key = jax.random.fold_in(key, 4127)
    key_len, key_pick, key_sign, key_perm, key_count, key_full, key_popular = jax.random.split(base_key, 7)
    half_len = RB_DEV // 2
    pair_count = ROWDEV // 2
    shifts = jax.random.randint(key_len, (pair_count,), -half_len, half_len + 1)
    forced = jax.random.randint(key_pick, (), 0, pair_count)
    flip_sign = jax.random.randint(key_sign, (), 0, 2) * 2 - 1
    shifts = jnp.where(jnp.arange(pair_count) == forced, half_len * flip_sign, shifts)
    lengths = jnp.stack([RB_DEV - shifts, RB_DEV + shifts], axis=1).reshape(ROWDEV).astype(jnp.int32)
    starts = jnp.cumsum(lengths) - lengths
    device_count = ROWDEV * COLDEV
    lattice_size = LMAX * COLUMN_BLOCKS_SET
    device_rows = jnp.arange(device_count) // COLDEV
    device_cols = jnp.arange(device_count) % COLDEV
    device_keys = jax.random.split(key_perm, device_count)
    popular_run = jax.random.randint(key_popular, (), 0, ROWDEV)
    prefers = jnp.arange(device_count) % 2 == 0

    def choose(dev_key, span_length, prefer):
        pairing_index = jax.random.permutation(dev_key, lattice_size)
        location_list = jnp.arange(lattice_size)
        favored_hosts = (pairing_index % COLUMN_BLOCKS_SET // GROUP == popular_run) & prefer
        extra_credit = jnp.where(favored_hosts, lattice_size, 0)
        rating_values = jnp.where(pairing_index // COLUMN_BLOCKS_SET < span_length, lattice_size - location_list + extra_credit, -1 - location_list)
        best_vals, best_idx = lax.top_k(rating_values, TILE_DEV)
        return pairing_index[best_idx]
    chosen = jax.vmap(choose)(device_keys, lengths[device_rows], prefers)
    row_list = starts[device_rows][:, None] + chosen // COLUMN_BLOCKS_SET
    col_local = chosen % COLUMN_BLOCKS_SET
    col_list = (col_local // GROUP * COLDEV + device_cols[:, None]) * GROUP + col_local % GROUP
    counts = TILE_DEV // jax.random.randint(key_count, (device_count,), 1, 5)
    full_dev = jax.random.randint(key_full, (), 0, device_count)
    counts = jnp.where(jnp.arange(device_count) == full_dev, TILE_DEV, counts)
    return (lengths, row_list.reshape(-1).astype(jnp.int32), col_list.reshape(-1).astype(jnp.int32), counts.astype(jnp.int32))


def draw_tile_blocks(key, part):
    fan_value = max(1, TB * TILE_DEV * COLDEV // (512 * RB_DEV))
    base_scale = float(fan_value) ** (-0.5)
    tile_total = ROWDEV * COLDEV * TILE_DEV
    owner_row = (jnp.arange(tile_total) // (COLDEV * TILE_DEV)).astype(jnp.float32)
    position = owner_row / float(ROWDEV - 1)
    draw_key = jax.random.fold_in(key, 9311)
    scales = base_scale * (0.5 + 1.5 * position)
    values = jnp.clip(jax.random.normal(draw_key, (tile_total, TB, TB), jnp.float32), -6.0, 6.0)
    return jnp.clip(values * scales[:, None, None], -8.0, 8.0).astype(jnp.bfloat16)


def draw_row_blocks(key, part):
    return tile_layout(key)[0]


def draw_tile_rows(key, part):
    return tile_layout(key)[1]


def draw_tile_cols(key, part):
    return tile_layout(key)[2]


def draw_tile_count(key, part):
    return tile_layout(key)[3]


def steps_of(own_key, dims, pieces, smallest, top_value):
    factor_of = 1.0
    for dim, parts in pieces:
        steps = jax.random.uniform(jax.random.fold_in(jax.random.fold_in(own_key, 6), dim), (parts,), jnp.float32, smallest / len(pieces), top_value / len(pieces))
        factor_of = factor_of * jnp.repeat(jnp.exp(steps), dims[dim] // parts).reshape((-1,) + (1,) * (len(dims) - 1 - dim))
    return factor_of


def gaussian(stream_key, shape, width, reach, cuts=(), held_as=jnp.bfloat16):
    entries = jax.random.normal(stream_key, shape, jnp.float32) * width
    if len(cuts) > 0:
        entries = steps_of(stream_key, shape, cuts, -0.22, 0.18) * entries
    return jnp.clip(entries, min=-reach, max=reach).astype(held_as)


def setup_inputs(seed: int = 0) -> dict:
    seeds = jax.random.split(jax.random.key(seed), 7)
    hub_seeds = gaussian(seeds[0], (ROWDEV * LMAX, K, TB), 1.0, 6.0, ((0, 32),))
    tile_blocks = draw_tile_blocks(jax.random.fold_in(seeds[6], 71), 0)
    tile_rows = draw_tile_rows(jax.random.fold_in(seeds[6], 71), 0)
    tile_cols = draw_tile_cols(jax.random.fold_in(seeds[6], 71), 0)
    tile_count = draw_tile_count(jax.random.fold_in(seeds[6], 71), 0)
    row_blocks = draw_row_blocks(jax.random.fold_in(seeds[6], 71), 0)
    return {"hub_seeds": hub_seeds, "tile_blocks": tile_blocks, "tile_rows": tile_rows, "tile_cols": tile_cols, "tile_count": tile_count, "row_blocks": row_blocks}


def normalize(raw_scores):
    squares = lax.optimization_barrier(jnp.sum(raw_scores * raw_scores, axis=(0, 2)))
    factor = 1.0 / jnp.sqrt(squares / HOSTS + 1.0)
    return (raw_scores * factor[None, :, None]).astype(jnp.bfloat16)

def rounded_partial(partial_value):
    return lax.optimization_barrier(partial_value.astype(jnp.bfloat16)).astype(jnp.float32)

def reference(hub_seeds, tile_blocks, tile_rows, tile_cols, tile_count, row_blocks):
    devices_all = ROWDEV * COLDEV
    starts = (jnp.cumsum(row_blocks) - row_blocks).astype(jnp.int32)
    slot_ids = jnp.arange(ROWDEV * LMAX, dtype=jnp.int32)
    usable = slot_ids % LMAX < row_blocks[slot_ids // LMAX]
    hub_now = jnp.where(usable[:, None, None], hub_seeds, jnp.zeros_like(hub_seeds))
    blocks_dev = tile_blocks.reshape(devices_all, TILE_DEV, TB, TB)
    owners = jnp.arange(devices_all, dtype=jnp.int32) // COLDEV
    rows_dev = tile_rows.reshape(devices_all, TILE_DEV)
    padded_rows = (owners[:, None] * LMAX + rows_dev - starts[owners][:, None]).astype(jnp.int32)
    cols_dev = tile_cols.reshape(devices_all, TILE_DEV)
    live_mask = (jnp.arange(TILE_DEV, dtype=jnp.int32)[None, :] < tile_count[:, None]).astype(jnp.float32)
    inputs_all = (blocks_dev, padded_rows, cols_dev, live_mask)
    authority = None
    for iteration in range(ITERS):

        def authority_step(running, inputs):
            blocks, row_ids, col_ids, weights = inputs
            picked = hub_now[row_ids].astype(jnp.float32)
            products = jnp.einsum('tkr,trc->tkc', picked, blocks.astype(jnp.float32))
            partial_value = jnp.zeros((NB, K, TB), jnp.float32).at[col_ids].add(products * weights[:, None, None])
            return (running + rounded_partial(partial_value), None)
        raw_authority, _ = lax.scan(authority_step, jnp.zeros((NB, K, TB), jnp.float32), inputs_all)
        authority = normalize(raw_authority)

        def hub_step(running, inputs):
            blocks, row_ids, col_ids, weights = inputs
            picked = authority[col_ids].astype(jnp.float32)
            products = jnp.einsum('tkc,trc->tkr', picked, blocks.astype(jnp.float32))
            partial_value = jnp.zeros((ROWDEV * LMAX, K, TB), jnp.float32).at[row_ids].add(products * weights[:, None, None])
            return (running + rounded_partial(partial_value), None)
        raw_hub, _ = lax.scan(hub_step, jnp.zeros((ROWDEV * LMAX, K, TB), jnp.float32), inputs_all)
        hub_now = normalize(raw_hub)
    return (authority, hub_now)
```

```python
import jax
import jax.numpy as jnp
from jax import lax
from jax.experimental import pallas as pl
from jax.experimental.pallas import tpu as pltpu
from jax.sharding import PartitionSpec as P

ITERS = 2
RB_DEV = 16
GROUP = 4
CHUNK = 32
UNROLL = 32
BF = jnp.bfloat16
F32 = jnp.float32


def coords(r):
    return {"x": r >> 3, "z": (r >> 1) & 3, "c": r & 1}


def side(v, dim):
    return (v & 1) ^ (v >> 1) if dim == "w" else v >> 1


def flip(v, dim):
    w, u = side(v, "w"), side(v, "u")
    if dim == "w":
        w ^= 1
    else:
        u ^= 1
    return u * 2 + (w ^ u)


def neighbour(r, dim):
    at = coords(r)
    if dim == "c":
        return r ^ 1
    at[dim[0]] = flip(at[dim[0]], dim[1])
    return at["x"] * 8 + at["z"] * 2 + at["c"]


ORDER = {
    (0, 0): ("xw", "zw", "xu", "zu"),
    (1, 0): ("zw", "xw", "zu", "xu"),
    (0, 1): ("xu", "zu", "xw", "zw"),
    (1, 1): ("zu", "xu", "zw", "xw"),
}
STEPS = 4


def swap(value, half, step):
    perm = [(r, neighbour(r, ORDER[(r & 1, half)][step])) for r in range(32)]
    return lax.ppermute(value, "row", perm)


def swap_core(value):
    return lax.ppermute(value, "row", [(r, r ^ 1) for r in range(32)])


def swap_y(value, step):
    perm = []
    for r in range(32):
        for y in range(4):
            dim = ("w", "u")[(r + step) % 2]
            perm.append((r * 4 + y, r * 4 + flip(y, dim)))
    return lax.ppermute(value, ("row", "col"), perm)


def positions(own_row, tile_cols):
    owner = tile_cols // RB_DEV
    inner = tile_cols % GROUP
    half = inner // 2
    core = owner & 1

    def bit(dim):
        shift = 3 if dim[0] == "x" else 1
        return side((owner >> shift) & 3, dim[1]) ^ side((own_row >> shift) & 3, dim[1])

    where = (core ^ (own_row & 1)) * 64 + half * 32 + inner % 2
    for step in range(STEPS):
        value = jnp.zeros_like(owner)
        for (c, h), dims in ORDER.items():
            value = jnp.where((core == c) & (half == h), bit(dims[step]), value)
        where = where + value * (16 >> step)
    return where


def split_sum(total, lane, first):
    out = jnp.zeros(total.shape[:1] + lane.shape[1:], BF)
    rest = total
    for part in range(3):
        piece = rest.astype(BF)
        rest = rest - piece.astype(F32)
        out = jnp.where(lane == first + part, piece, out)
    return out


def start_tiles(count, tiles, buf, sems):
    for c in range(tiles.shape[0] // CHUNK):

        @pl.when(c * CHUNK < count)
        def _():
            rows = pl.ds(c * CHUNK, CHUNK)
            pltpu.make_async_copy(tiles.at[rows], buf.at[rows], sems.at[c]).start()


def over_tiles(count, tiles, buf, sems, group):
    def chunk(c, carry):
        rows = pl.ds(c * CHUNK, CHUNK)
        pltpu.make_async_copy(tiles.at[rows], buf.at[rows], sems.at[c]).wait()
        for g in range(CHUNK // UNROLL):
            group(c * CHUNK + g * UNROLL)
        return carry

    lax.fori_loop(0, (count + CHUNK - 1) // CHUNK, chunk, 0)


def authority_body(index, hub, tiles, keep, send, buf, acc, sems, *, with_sum):
    slots = tiles.shape[0]
    count = index[slots]
    start_tiles(count, tiles, buf, sems)
    acc[...] = jnp.zeros_like(acc)

    def group(first):
        terms = []
        for u in range(UNROLL):
            slot = index[first + u] & 255
            terms.append(jnp.dot(hub[slot], buf[first + u], preferred_element_type=F32))
        for u in range(UNROLL):
            where = index[first + u] >> 16
            acc[where] = acc[where] + terms[u]

    over_tiles(count, tiles, buf, sems, group)
    keep[:64] = acc[:64].astype(BF)
    send[:64] = acc[64:128].astype(BF)
    if with_sum:
        squares = jnp.zeros(hub.shape[1:], F32)
        for s in range(hub.shape[0]):
            values = hub[s].astype(F32)
            squares = squares + values * values
        total = jnp.sum(squares, axis=1, keepdims=True)
        lane = lax.broadcasted_iota(jnp.int32, squares.shape, 1)
        block = split_sum(total, lane, 3 * index[slots + 1])
        keep[64] = block
        send[64] = block


def hub_body(index, p0, p1, p2, p3, tiles, out, buf, acc, gathered, sems):
    slots = tiles.shape[0]
    count = index[slots]
    start_tiles(count, tiles, buf, sems)
    acc[...] = jnp.zeros_like(acc)

    def take(b, squares):
        for q, piece in enumerate((p0, p1, p2, p3)):
            block = piece[b]
            gathered[q * 32 + b] = block
            values = block.astype(F32)
            squares = squares + values * values
        return squares

    squares = lax.fori_loop(0, 32, take, jnp.zeros(p0.shape[1:], F32))
    total = jnp.sum(squares, axis=1, keepdims=True)
    lane = lax.broadcasted_iota(jnp.int32, squares.shape, 1)
    out[out.shape[0] - 1] = split_sum(total, lane, 3 * index[slots + 2])

    def group(first):
        terms = []
        for u in range(UNROLL):
            where = jnp.minimum(index[first + u] >> 16, 127)
            terms.append(
                lax.dot_general(
                    gathered[where],
                    buf[first + u],
                    (((1,), (1,)), ((), ())),
                    preferred_element_type=F32,
                )
            )
        for u in range(UNROLL):
            slot = (index[first + u] >> 8) & 255
            acc[slot] = acc[slot] + terms[u]

    over_tiles(count, tiles, buf, sems, group)
    out[: out.shape[0] - 1] = acc[: out.shape[0] - 1].astype(BF)


SMEM = pl.BlockSpec(memory_space=pltpu.SMEM)
VMEM = pl.BlockSpec(memory_space=pltpu.VMEM)
HBM = pl.BlockSpec(memory_space=pl.ANY)
PARAMS = pltpu.CompilerParams(vmem_limit_bytes=48 * 2**20)


def authority_terms(index, hub, tiles, with_sum):
    count, side_len, _ = tiles.shape
    vectors = hub.shape[1]
    shape = jax.ShapeDtypeStruct((65 if with_sum else 64, vectors, side_len), BF)

    def body(*refs):
        authority_body(*refs, with_sum=with_sum)

    return pl.pallas_call(
        body,
        name="authority_terms",
        in_specs=[SMEM, VMEM, HBM],
        out_specs=[VMEM, VMEM],
        out_shape=[shape, shape],
        scratch_shapes=[
            pltpu.VMEM(tiles.shape, BF),
            pltpu.VMEM((129, vectors, side_len), F32),
            pltpu.SemaphoreType.DMA((count // CHUNK,)),
        ],
        compiler_params=PARAMS,
        cost_estimate=pl.CostEstimate(
            flops=2 * count * vectors * side_len**2, bytes_accessed=tiles.size * 2, transcendentals=0
        ),
    )(index, hub, tiles)


def hub_terms(index, pieces, tiles, slot_count):
    count, side_len, _ = tiles.shape
    vectors = pieces[0].shape[1]
    return pl.pallas_call(
        hub_body,
        name="hub_terms",
        in_specs=[SMEM, VMEM, VMEM, VMEM, VMEM, HBM],
        out_specs=VMEM,
        out_shape=jax.ShapeDtypeStruct((slot_count + 1, vectors, side_len), BF),
        scratch_shapes=[
            pltpu.VMEM(tiles.shape, BF),
            pltpu.VMEM((slot_count + 1, vectors, side_len), F32),
            pltpu.VMEM((128, vectors, side_len), BF),
            pltpu.SemaphoreType.DMA((count // CHUNK,)),
        ],
        compiler_params=PARAMS,
        cost_estimate=pl.CostEstimate(
            flops=2 * count * vectors * side_len**2, bytes_accessed=tiles.size * 2, transcendentals=0
        ),
    )(index, *pieces, tiles)


def added(a, b):
    return a.astype(F32) + b.astype(F32)


def reduce_to_owner(keep, send, with_sum):
    mine = added(keep, swap_core(send)).astype(BF)
    halves = [mine[:32], mine[32:64]]
    total = mine[64:] if with_sum else None
    for step in range(STEPS):
        size = 16 >> step
        for half in range(2):
            value = halves[half]
            out = value[size:]
            if with_sum and half == 0:
                out = jnp.concatenate([out, total])
            got = swap(out, half, step)
            if with_sum and half == 0:
                total = added(total, got[size:]).astype(BF)
                got = got[:size]
            value = added(value[:size], got)
            halves[half] = value if step == STEPS - 1 else value.astype(BF)
    return jnp.concatenate(halves), total


def gather_from_owners(own):
    halves = [own[:2], own[2:]]
    for step in reversed(range(STEPS)):
        for half in range(2):
            value = halves[half]
            halves[half] = jnp.concatenate([value, swap(value, half, step)])
    return (*halves, *(swap_core(value) for value in halves))


def local(hub_seeds, tile_blocks, tile_rows, tile_cols, tile_count, row_blocks):
    own_row = lax.axis_index("row")
    own_col = lax.axis_index("col")
    slot_count = hub_seeds.shape[0]
    tile_slots = tile_blocks.shape[0]
    host_count = RB_DEV * row_blocks.shape[0] * tile_blocks.shape[1]
    before = jnp.arange(row_blocks.shape[0], dtype=jnp.int32) < own_row
    first_block = jnp.sum(jnp.where(before, row_blocks, 0))
    live = jnp.arange(tile_slots, dtype=jnp.int32) < tile_count[0]
    slot = jnp.clip(tile_rows - first_block, 0, slot_count - 1)
    to_slot = jnp.where(live, slot, slot_count)
    where = jnp.where(live, positions(own_row, tile_cols), 128)
    packed = slot + to_slot * 256 + where * 65536
    tail = jnp.zeros((128,), jnp.int32)
    tail = jnp.where(jnp.arange(128) == 0, tile_count[0], tail)
    tail = jnp.where(jnp.arange(128) == 1, own_row, tail)
    tail = jnp.where(jnp.arange(128) == 2, own_col, tail)
    index = jnp.concatenate([packed, tail])
    usable = jnp.arange(slot_count, dtype=jnp.int32) < row_blocks[own_row]
    hub = jnp.where(usable[:, None, None], hub_seeds, jnp.zeros_like(hub_seeds))
    for iteration in range(ITERS):
        with_sum = iteration > 0
        keep, send = authority_terms(index, hub, tile_blocks, with_sum)
        own, hub_total = reduce_to_owner(keep, send, with_sum)
        if with_sum:
            squares = jnp.sum(hub_total.astype(F32), axis=(0, 2))
            own = own * (1.0 / jnp.sqrt(squares / host_count + 1.0))[None, :, None]
        pieces = gather_from_owners(own.astype(BF))
        terms = hub_terms(index, pieces, tile_blocks, slot_count)
        terms = added(terms, swap_y(terms, 0)).astype(BF)
        terms = added(terms, swap_y(terms, 1))
        squares = jnp.sum(terms[slot_count], axis=1)
        factor = (1.0 / jnp.sqrt(squares / host_count + 1.0))[None, :, None]
        raw_hub = terms[:slot_count] * factor
        hub = raw_hub.astype(BF)
    authority = (own * factor).astype(BF)
    squares = jnp.sum(raw_hub * raw_hub, axis=(0, 2))
    squares = squares + swap_core(squares)
    for step in range(STEPS):
        squares = squares + swap(squares, 0, step)
    factor = (1.0 / jnp.sqrt(squares / host_count + 1.0))[None, :, None]
    return authority, (raw_hub * factor).astype(BF)


def solution(mesh):
    both = ("row", "col")
    return jax.shard_map(
        local,
        mesh=mesh,
        in_specs=(P("row"), P(both), P(both), P(both), P(both), P()),
        out_specs=(P(both), P("row")),
        check_vma=False,
    )
```

```python
import jax
import jax.numpy as jnp
from jax import lax
from jax.experimental import pallas as pl
from jax.experimental.pallas import tpu as pltpu
from jax.sharding import PartitionSpec as P

ITERS = 2
RB_DEV = 16
GROUP = 4
CHUNK = 64
BF = jnp.bfloat16
F32 = jnp.float32

FAR_FIRST = (2, 1, 3)


def moved(r, step, k):
    x, z, c = r >> 3, (r >> 1) & 3, r & 1
    if (c + step) % 2 == 0:
        x = (x + k) % 4
    else:
        z = (z + k) % 4
    return x * 8 + z * 2 + c


def shift(value, step, k):
    return lax.ppermute(value, "row", [(r, moved(r, step, k)) for r in range(32)])


def swap_core(value):
    return lax.ppermute(value, "row", [(r, r ^ 1) for r in range(32)])


def swap_y(value, step):
    perm = []
    for r in range(32):
        for y in range(4):
            to = y ^ 1 if (r + step) % 2 == 0 else 3 - y
            perm.append((r * 4 + y, r * 4 + to))
    return lax.ppermute(value, ("row", "col"), perm)


def positions(own_row, tile_cols):
    owner = tile_cols // RB_DEV
    core = owner & 1
    away_x = ((owner >> 3) - (own_row >> 3)) & 3
    away_z = ((owner >> 1) - (own_row >> 1)) & 3
    first = jnp.where(core == 0, away_x, away_z)
    second = jnp.where(core == 0, away_z, away_x)
    return (core ^ (own_row & 1)) * 64 + first * 16 + second * 4 + tile_cols % GROUP


def split_sum(total, lane, first):
    out = jnp.zeros(total.shape[:1] + lane.shape[1:], BF)
    rest = total
    for part in range(3):
        piece = rest.astype(BF)
        rest = rest - piece.astype(F32)
        out = jnp.where(lane == first + part, piece, out)
    return out


def start_tiles(count, tiles, buf, sems):
    for c in range(tiles.shape[0] // CHUNK):

        @pl.when(c * CHUNK < count)
        def _():
            rows = pl.ds(c * CHUNK, CHUNK)
            pltpu.make_async_copy(tiles.at[rows], buf.at[rows], sems.at[c]).start()


def over_tiles(count, tiles, buf, sems, group):
    def chunk(c, carry):
        rows = pl.ds(c * CHUNK, CHUNK)
        pltpu.make_async_copy(tiles.at[rows], buf.at[rows], sems.at[c]).wait()
        group(c * CHUNK)
        return carry

    lax.fori_loop(0, (count + CHUNK - 1) // CHUNK, chunk, 0)


def authority_body(index, hub, tiles, keep, send, buf, acc, sems, *, with_sum):
    slots = tiles.shape[0]
    count = index[slots]
    start_tiles(count, tiles, buf, sems)
    acc[...] = jnp.zeros_like(acc)

    def group(first):
        terms = []
        for u in range(CHUNK):
            slot = index[first + u] & 255
            terms.append(jnp.dot(hub[slot], buf[first + u], preferred_element_type=F32))
        for u in range(CHUNK):
            where = index[first + u] >> 16
            acc[where] = acc[where] + terms[u]

    over_tiles(count, tiles, buf, sems, group)
    keep[:64] = acc[:64].astype(BF)
    send[:64] = acc[64:128].astype(BF)
    if with_sum:
        squares = jnp.zeros(hub.shape[1:], F32)
        for s in range(hub.shape[0]):
            values = hub[s].astype(F32)
            squares = squares + values * values
        total = jnp.sum(squares, axis=1, keepdims=True)
        lane = lax.broadcasted_iota(jnp.int32, squares.shape, 1)
        block = split_sum(total, lane, 3 * index[slots + 1])
        keep[64] = block
        send[64] = block


def hub_body(index, *refs):
    *pieces, tiles, out, buf, acc, gathered, sems = refs
    slots = tiles.shape[0]
    count = index[slots]
    start_tiles(count, tiles, buf, sems)
    acc[...] = jnp.zeros_like(acc)
    size = pieces[0].shape[0]

    def take(b, squares):
        for q, piece in enumerate(pieces):
            block = piece[b]
            gathered[q * size + b] = block
            values = block.astype(F32)
            squares = squares + values * values
        return squares

    squares = lax.fori_loop(0, size, take, jnp.zeros(pieces[0].shape[1:], F32))
    total = jnp.sum(squares, axis=1, keepdims=True)
    lane = lax.broadcasted_iota(jnp.int32, squares.shape, 1)
    out[out.shape[0] - 1] = split_sum(total, lane, 3 * index[slots + 2])

    def group(first):
        terms = []
        for u in range(CHUNK):
            where = jnp.minimum(index[first + u] >> 16, 127)
            terms.append(
                lax.dot_general(
                    buf[first + u],
                    gathered[where],
                    (((1,), (1,)), ((), ())),
                    preferred_element_type=F32,
                )
            )
        for u in range(CHUNK):
            slot = (index[first + u] >> 8) & 255
            acc[slot] = acc[slot] + terms[u]

    over_tiles(count, tiles, buf, sems, group)
    for s in range(out.shape[0] - 1):
        out[s] = acc[s].T.astype(BF)


SMEM = pl.BlockSpec(memory_space=pltpu.SMEM)
VMEM = pl.BlockSpec(memory_space=pltpu.VMEM)
HBM = pl.BlockSpec(memory_space=pl.ANY)
PARAMS = pltpu.CompilerParams(vmem_limit_bytes=48 * 2**20)


def authority_terms(index, hub, tiles, with_sum):
    count, side_len, _ = tiles.shape
    vectors = hub.shape[1]
    shape = jax.ShapeDtypeStruct((65 if with_sum else 64, vectors, side_len), BF)

    def body(*refs):
        authority_body(*refs, with_sum=with_sum)

    return pl.pallas_call(
        body,
        name="authority_terms",
        in_specs=[SMEM, VMEM, HBM],
        out_specs=[VMEM, VMEM],
        out_shape=[shape, shape],
        scratch_shapes=[
            pltpu.VMEM(tiles.shape, BF),
            pltpu.VMEM((129, vectors, side_len), F32),
            pltpu.SemaphoreType.DMA((count // CHUNK,)),
        ],
        compiler_params=PARAMS,
        cost_estimate=pl.CostEstimate(
            flops=2 * count * vectors * side_len**2, bytes_accessed=tiles.size * 2, transcendentals=0
        ),
    )(index, hub, tiles)


def hub_terms(index, pieces, tiles, slot_count):
    count, side_len, _ = tiles.shape
    vectors = pieces[0].shape[1]
    return pl.pallas_call(
        hub_body,
        name="hub_terms",
        in_specs=[SMEM] + [VMEM] * len(pieces) + [HBM],
        out_specs=VMEM,
        out_shape=jax.ShapeDtypeStruct((slot_count + 1, vectors, side_len), BF),
        scratch_shapes=[
            pltpu.VMEM(tiles.shape, BF),
            pltpu.VMEM((slot_count + 1, side_len, vectors), F32),
            pltpu.VMEM((128, vectors, side_len), BF),
            pltpu.SemaphoreType.DMA((count // CHUNK,)),
        ],
        compiler_params=PARAMS,
        cost_estimate=pl.CostEstimate(
            flops=2 * count * vectors * side_len**2, bytes_accessed=tiles.size * 2, transcendentals=0
        ),
    )(index, *pieces, tiles)


def added(a, b):
    return a.astype(F32) + b.astype(F32)


def reduce_to_owner(keep, send, with_sum):
    mine = added(keep, swap_core(send))
    total = mine[64:] if with_sum else None
    mine = mine[:64]
    for step in range(2):
        size = mine.shape[0] // 4
        got = {}
        for k in FAR_FIRST:
            out = mine[k * size : (k + 1) * size]
            if with_sum:
                out = jnp.concatenate([out, total])
            got[k] = shift(out.astype(BF), step, k).astype(F32)
        mine = mine[:size] + got[1][:size] + got[2][:size] + got[3][:size]
        if with_sum:
            total = total + got[1][size:] + got[2][size:] + got[3][size:]
    return mine, total


def gather_from_owners(own):
    got = {k: shift(own, 1, -k) for k in FAR_FIRST}
    mine = jnp.concatenate([own, got[1], got[2], got[3]])
    got = {k: shift(mine, 0, -k) for k in FAR_FIRST}
    half = [mine, got[1], got[2], got[3]]
    return half + [swap_core(piece) for piece in half]


def local(hub_seeds, tile_blocks, tile_rows, tile_cols, tile_count, row_blocks):
    own_row = lax.axis_index("row")
    own_col = lax.axis_index("col")
    slot_count = hub_seeds.shape[0]
    tile_slots = tile_blocks.shape[0]
    host_count = RB_DEV * row_blocks.shape[0] * tile_blocks.shape[1]
    before = jnp.arange(row_blocks.shape[0], dtype=jnp.int32) < own_row
    first_block = jnp.sum(jnp.where(before, row_blocks, 0))
    live = jnp.arange(tile_slots, dtype=jnp.int32) < tile_count[0]
    slot = jnp.clip(tile_rows - first_block, 0, slot_count - 1)
    to_slot = jnp.where(live, slot, slot_count)
    where = jnp.where(live, positions(own_row, tile_cols), 128)
    packed = slot + to_slot * 256 + where * 65536
    tail = jnp.zeros((128,), jnp.int32)
    tail = jnp.where(jnp.arange(128) == 0, tile_count[0], tail)
    tail = jnp.where(jnp.arange(128) == 1, own_row, tail)
    tail = jnp.where(jnp.arange(128) == 2, own_col, tail)
    index = jnp.concatenate([packed, tail])
    usable = jnp.arange(slot_count, dtype=jnp.int32) < row_blocks[own_row]
    hub = jnp.where(usable[:, None, None], hub_seeds, jnp.zeros_like(hub_seeds))
    for iteration in range(ITERS):
        with_sum = iteration > 0
        keep, send = authority_terms(index, hub, tile_blocks, with_sum)
        own, hub_total = reduce_to_owner(keep, send, with_sum)
        if with_sum:
            squares = jnp.sum(hub_total.astype(F32), axis=(0, 2))
            own = own * (1.0 / jnp.sqrt(squares / host_count + 1.0))[None, :, None]
        pieces = gather_from_owners(own.astype(BF))
        terms = hub_terms(index, pieces, tile_blocks, slot_count)
        terms = added(terms, swap_y(terms, 0)).astype(BF)
        terms = added(terms, swap_y(terms, 1))
        squares = jnp.sum(terms[slot_count], axis=1)
        factor = (1.0 / jnp.sqrt(squares / host_count + 1.0))[None, :, None]
        raw_hub = terms[:slot_count] * factor
        hub = raw_hub.astype(BF)
    authority = (own * factor).astype(BF)
    squares = jnp.sum(raw_hub * raw_hub, axis=(0, 2))
    squares = squares + swap_core(squares)
    for step in range(2):
        got = {k: shift(squares, step, k) for k in FAR_FIRST}
        squares = (squares + got[2]) + (got[1] + got[3])
    factor = (1.0 / jnp.sqrt(squares / host_count + 1.0))[None, :, None]
    return authority, (raw_hub * factor).astype(BF)


def solution(mesh):
    both = ("row", "col")
    return jax.shard_map(
        local,
        mesh=mesh,
        in_specs=(P("row"), P(both), P(both), P(both), P(both), P()),
        out_specs=(P(both), P("row")),
        check_vma=False,
    )
```

```python
import jax
import jax.numpy as jnp
from jax import lax
from jax.experimental import pallas as pl
from jax.experimental.pallas import tpu as pltpu
from jax.sharding import PartitionSpec as P

ITERS = 2
RB_DEV = 16
GROUP = 4
CHUNK = 96
AHEAD = 3
BF = jnp.bfloat16
F32 = jnp.float32

FAR_FIRST = (2, 1, 3)


def moved(r, step, k):
    x, z, c = r >> 3, (r >> 1) & 3, r & 1
    if (c + step) % 2 == 0:
        x = (x + k) % 4
    else:
        z = (z + k) % 4
    return x * 8 + z * 2 + c


def shift(value, step, k):
    return lax.ppermute(value, "row", [(r, moved(r, step, k)) for r in range(32)])


def swap_core(value):
    return lax.ppermute(value, "row", [(r, r ^ 1) for r in range(32)])


def swap_y(value, step):
    perm = []
    for r in range(32):
        for y in range(4):
            to = y ^ 1 if (r + step) % 2 == 0 else 3 - y
            perm.append((r * 4 + y, r * 4 + to))
    return lax.ppermute(value, ("row", "col"), perm)


def positions(own_row, tile_cols):
    owner = tile_cols // RB_DEV
    core = owner & 1
    at_x, at_z = owner >> 3, (owner >> 1) & 3
    first = jnp.where(core == 0, at_x - (own_row >> 3), at_z - (own_row >> 1)) & 3
    second = jnp.where(core == 0, at_z, at_x)
    return (core ^ (own_row & 1)) * 64 + first * 16 + second * 4 + tile_cols % GROUP


def split_sum(total, lane, first):
    out = jnp.zeros(total.shape[:1] + lane.shape[1:], BF)
    rest = total
    for part in range(3):
        piece = rest.astype(BF)
        rest = rest - piece.astype(F32)
        out = jnp.where(lane == first + part, piece, out)
    return out


def over_tiles(count, tiles, buf, sems, prepare, group):
    chunks = (count + CHUNK - 1) // CHUNK

    def copy(c):
        rows = pl.ds(c * CHUNK, CHUNK)
        return pltpu.make_async_copy(tiles.at[rows], buf.at[rows], sems.at[c])

    for c in range(AHEAD):

        @pl.when(c < chunks)
        def _():
            copy(c).start()

    prepare()

    def step(c, carry):
        @pl.when(c + AHEAD < chunks)
        def _():
            copy(c + AHEAD).start()

        copy(c).wait()
        group(c * CHUNK)
        return carry

    lax.fori_loop(0, chunks, step, 0)


def authority_body(index, hub, tiles, keep, send, buf, acc, used, sems, *, with_sum):
    slots = tiles.shape[0]
    count = index[slots]

    def prepare():
        acc[...] = jnp.zeros_like(acc)
        for s in range(hub.shape[0]):
            used[s] = jnp.where(s < index[slots + 3], hub[s], jnp.zeros_like(hub[s]))

    def group(first):
        terms = []
        for u in range(CHUNK):
            slot = index[first + u] & 255
            terms.append(jnp.dot(used[slot], buf[first + u], preferred_element_type=F32))
        for u in range(CHUNK):
            where = index[first + u] >> 16
            acc[where] = acc[where] + terms[u]

    over_tiles(count, tiles, buf, sems, prepare, group)
    keep[:64] = acc[:64].astype(BF)
    send[:64] = acc[64:128].astype(BF)
    if with_sum:
        squares = jnp.zeros(hub.shape[1:], F32)
        for s in range(hub.shape[0]):
            values = used[s].astype(F32)
            squares = squares + values * values
        total = jnp.sum(squares, axis=1, keepdims=True)
        lane = lax.broadcasted_iota(jnp.int32, squares.shape, 1)
        block = split_sum(total, lane, 3 * index[slots + 1])
        keep[64] = block
        send[64] = block


def hub_body(index, *refs):
    *pieces, tiles, out, buf, acc, gathered, sems = refs
    slots = tiles.shape[0]
    count = index[slots]
    size = pieces[0].shape[0]

    def prepare():
        acc[...] = jnp.zeros_like(acc)

        def take(b, squares):
            for q, piece in enumerate(pieces):
                block = piece[b]
                gathered[q * size + b] = block
                values = block.astype(F32)
                squares = squares + values * values
            return squares

        squares = lax.fori_loop(0, size, take, jnp.zeros(pieces[0].shape[1:], F32))
        total = jnp.sum(squares, axis=1, keepdims=True)
        lane = lax.broadcasted_iota(jnp.int32, squares.shape, 1)
        out[out.shape[0] - 1] = split_sum(total, lane, 3 * index[slots + 2])

    def group(first):
        terms = []
        for u in range(CHUNK):
            where = jnp.minimum(index[first + u] >> 16, 127)
            terms.append(
                lax.dot_general(
                    buf[first + u],
                    gathered[where],
                    (((1,), (1,)), ((), ())),
                    preferred_element_type=F32,
                )
            )
        for u in range(CHUNK):
            slot = (index[first + u] >> 8) & 255
            acc[slot] = acc[slot] + terms[u]

    over_tiles(count, tiles, buf, sems, prepare, group)
    for s in range(out.shape[0] - 1):
        out[s] = acc[s].T.astype(BF)


SMEM = pl.BlockSpec(memory_space=pltpu.SMEM)
VMEM = pl.BlockSpec(memory_space=pltpu.VMEM)
HBM = pl.BlockSpec(memory_space=pl.ANY)
PARAMS = pltpu.CompilerParams(vmem_limit_bytes=48 * 2**20)


def authority_terms(index, hub, tiles, with_sum):
    count, side_len, _ = tiles.shape
    vectors = hub.shape[1]
    shape = jax.ShapeDtypeStruct((65 if with_sum else 64, vectors, side_len), BF)

    def body(*refs):
        authority_body(*refs, with_sum=with_sum)

    return pl.pallas_call(
        body,
        name="authority_terms",
        in_specs=[SMEM, VMEM, HBM],
        out_specs=[VMEM, VMEM],
        out_shape=[shape, shape],
        scratch_shapes=[
            pltpu.VMEM(tiles.shape, BF),
            pltpu.VMEM((129, vectors, side_len), F32),
            pltpu.VMEM(hub.shape, BF),
            pltpu.SemaphoreType.DMA((count // CHUNK,)),
        ],
        compiler_params=PARAMS,
        cost_estimate=pl.CostEstimate(
            flops=2 * count * vectors * side_len**2, bytes_accessed=tiles.size * 2, transcendentals=0
        ),
    )(index, hub, tiles)


def hub_terms(index, pieces, tiles, slot_count):
    count, side_len, _ = tiles.shape
    vectors = pieces[0].shape[1]
    return pl.pallas_call(
        hub_body,
        name="hub_terms",
        in_specs=[SMEM] + [VMEM] * len(pieces) + [HBM],
        out_specs=VMEM,
        out_shape=jax.ShapeDtypeStruct((slot_count + 1, vectors, side_len), BF),
        scratch_shapes=[
            pltpu.VMEM(tiles.shape, BF),
            pltpu.VMEM((slot_count + 1, side_len, vectors), F32),
            pltpu.VMEM((128, vectors, side_len), BF),
            pltpu.SemaphoreType.DMA((count // CHUNK,)),
        ],
        compiler_params=PARAMS,
        cost_estimate=pl.CostEstimate(
            flops=2 * count * vectors * side_len**2, bytes_accessed=tiles.size * 2, transcendentals=0
        ),
    )(index, *pieces, tiles)


def added(a, b):
    return a.astype(F32) + b.astype(F32)


def reduce_over_plane(keep, send, with_sum):
    both = added(keep, swap_core(send))
    extra = [both[64:]] if with_sum else []
    size = 16
    out = {k: [both[k * size : (k + 1) * size]] + extra for k in FAR_FIRST}
    got = {k: shift(jnp.concatenate(out[k]).astype(BF), 0, k).astype(F32) for k in FAR_FIRST}
    mine = jnp.concatenate([both[:size]] + extra)
    mine = (mine + got[1] + got[2] + got[3]).astype(BF)
    got = {k: shift(mine, 1, k).astype(F32) for k in FAR_FIRST}
    mine = (mine.astype(F32) + got[2]) + (got[1] + got[3])
    return mine[:size], mine[size:]


def gather_over_ring(mine):
    got = {k: shift(mine, 0, -k) for k in FAR_FIRST}
    half = [mine, got[1], got[2], got[3]]
    return half + [swap_core(piece) for piece in half]


def local(hub_seeds, tile_blocks, tile_rows, tile_cols, tile_count, row_blocks):
    own_row = lax.axis_index("row")
    own_col = lax.axis_index("col")
    slot_count = hub_seeds.shape[0]
    tile_slots = tile_blocks.shape[0]
    host_count = RB_DEV * row_blocks.shape[0] * tile_blocks.shape[1]
    ranges = jnp.arange(row_blocks.shape[0], dtype=jnp.int32)
    first_block = jnp.sum(jnp.where(ranges < own_row, row_blocks, 0))
    usable = jnp.sum(jnp.where(ranges == own_row, row_blocks, 0))
    live = jnp.arange(tile_slots, dtype=jnp.int32) < tile_count[0]
    slot = jnp.clip(tile_rows - first_block, 0, slot_count - 1)
    to_slot = jnp.where(live, slot, slot_count)
    where = jnp.where(live, positions(own_row, tile_cols), 128)
    packed = slot + to_slot * 256 + where * 65536
    tail = jnp.zeros((128,), jnp.int32)
    tail = jnp.where(jnp.arange(128) == 0, tile_count[0], tail)
    tail = jnp.where(jnp.arange(128) == 1, own_row, tail)
    tail = jnp.where(jnp.arange(128) == 2, own_col, tail)
    tail = jnp.where(jnp.arange(128) == 3, usable, tail)
    index = jnp.concatenate([packed, tail])
    hub = hub_seeds
    for iteration in range(ITERS):
        with_sum = iteration > 0
        keep, send = authority_terms(index, hub, tile_blocks, with_sum)
        ring, hub_total = reduce_over_plane(keep, send, with_sum)
        if with_sum:
            squares = jnp.sum(hub_total.astype(F32), axis=(0, 2))
            ring = ring * (1.0 / jnp.sqrt(squares / host_count + 1.0))[None, :, None]
        pieces = gather_over_ring(ring.astype(BF))
        terms = hub_terms(index, pieces, tile_blocks, slot_count)
        terms = added(terms, swap_y(terms, 0)).astype(BF)
        terms = added(terms, swap_y(terms, 1))
        squares = jnp.sum(terms[slot_count], axis=1)
        factor = (1.0 / jnp.sqrt(squares / host_count + 1.0))[None, :, None]
        raw_hub = terms[:slot_count] * factor
        hub = raw_hub.astype(BF)
    second = jnp.where((own_row & 1) == 0, (own_row >> 1) & 3, own_row >> 3)
    own = lax.dynamic_slice_in_dim(ring, second * GROUP, GROUP)
    authority = (own * factor).astype(BF)
    squares = jnp.sum(raw_hub * raw_hub, axis=(0, 2))
    squares = squares + swap_core(squares)
    for step in range(2):
        got = {k: shift(squares, step, k) for k in FAR_FIRST}
        squares = (squares + got[2]) + (got[1] + got[3])
    factor = (1.0 / jnp.sqrt(squares / host_count + 1.0))[None, :, None]
    return authority, (raw_hub * factor).astype(BF)


def solution(mesh):
    both = ("row", "col")
    return jax.shard_map(
        local,
        mesh=mesh,
        in_specs=(P("row"), P(both), P(both), P(both), P(both), P()),
        out_specs=(P(both), P("row")),
        check_vma=False,
    )
```

```python
import jax
import jax.numpy as jnp
from jax import lax
from jax.experimental import pallas as pl
from jax.experimental.pallas import tpu as pltpu
from jax.sharding import PartitionSpec as P

ITERS = 2
RB_DEV = 16
GROUP = 4
CHUNK = 96
PIECE = 32
AHEAD = 9
BF = jnp.bfloat16
F32 = jnp.float32

FAR_FIRST = (2, 1, 3)


def moved(r, step, k):
    x, z, c = r >> 3, (r >> 1) & 3, r & 1
    if (c + step) % 2 == 0:
        x = (x + k) % 4
    else:
        z = (z + k) % 4
    return x * 8 + z * 2 + c


def shift(value, step, k):
    return lax.ppermute(value, "row", [(r, moved(r, step, k)) for r in range(32)])


def swap_core(value):
    return lax.ppermute(value, "row", [(r, r ^ 1) for r in range(32)])


def swap_y(value, step):
    perm = []
    for r in range(32):
        for y in range(4):
            to = y ^ 1 if (r + step) % 2 == 0 else 3 - y
            perm.append((r * 4 + y, r * 4 + to))
    return lax.ppermute(value, ("row", "col"), perm)


def positions(own_row, tile_cols):
    owner = tile_cols // RB_DEV
    core = owner & 1
    at_x, at_z = owner >> 3, (owner >> 1) & 3
    first = jnp.where(core == 0, at_x - (own_row >> 3), at_z - (own_row >> 1)) & 3
    second = jnp.where(core == 0, at_z, at_x)
    return (core ^ (own_row & 1)) * 64 + first * 16 + second * 4 + tile_cols % GROUP


def split_sum(total, lane, first):
    out = jnp.zeros(total.shape[:1] + lane.shape[1:], BF)
    rest = total
    for part in range(3):
        piece = rest.astype(BF)
        rest = rest - piece.astype(F32)
        out = jnp.where(lane == first + part, piece, out)
    return out


def over_tiles(count, tiles, buf, sems, prepare, product, add):
    chunks = (count + CHUNK - 1) // CHUNK
    pieces = chunks * (CHUNK // PIECE)

    def copy(p):
        rows = pl.ds(p * PIECE, PIECE)
        return pltpu.make_async_copy(tiles.at[rows], buf.at[rows], sems.at[p])

    for p in range(AHEAD):

        @pl.when(p < pieces)
        def _():
            copy(p).start()

    prepare()

    def step(c, carry):
        first = c * (CHUNK // PIECE)

        @pl.when(c + AHEAD * PIECE // CHUNK < chunks)
        def _():
            for q in range(CHUNK // PIECE):
                copy(first + AHEAD + q).start()

        terms = []
        for q in range(CHUNK // PIECE):
            copy(first + q).wait()
            for u in range(PIECE):
                terms.append(product((first + q) * PIECE + u))
        for u in range(CHUNK):
            add(c * CHUNK + u, terms[u])
        return carry

    lax.fori_loop(0, chunks, step, 0)


def authority_body(index, hub, tiles, keep, send, buf, acc, used, sems):
    slots = tiles.shape[0]

    def prepare():
        acc[...] = jnp.zeros_like(acc)
        for s in range(hub.shape[0]):
            used[s] = jnp.where(s < index[slots + 3], hub[s], jnp.zeros_like(hub[s]))

    def product(t):
        return jnp.dot(used[index[t] & 255], buf[t], preferred_element_type=F32)

    def add(t, term):
        where = index[t] >> 16
        acc[where] = acc[where] + term

    over_tiles(index[slots], tiles, buf, sems, prepare, product, add)
    keep[...] = acc[:64].astype(BF)
    send[...] = acc[64:128].astype(BF)


def hub_body(index, *refs):
    *pieces, tiles, out, buf, acc, gathered, sems = refs
    slots = tiles.shape[0]
    size = pieces[0].shape[0]

    def prepare():
        acc[...] = jnp.zeros_like(acc)

        def take(b, squares):
            for q, piece in enumerate(pieces):
                block = piece[b]
                gathered[q * size + b] = block
                values = block.astype(F32)
                squares = squares + values * values
            return squares

        squares = lax.fori_loop(0, size, take, jnp.zeros(pieces[0].shape[1:], F32))
        total = jnp.sum(squares, axis=1, keepdims=True)
        lane = lax.broadcasted_iota(jnp.int32, squares.shape, 1)
        out[out.shape[0] - 1] = split_sum(total, lane, 3 * index[slots + 2])

    def product(t):
        block = gathered[jnp.minimum(index[t] >> 16, 127)]
        return lax.dot_general(
            buf[t], block, (((1,), (1,)), ((), ())), preferred_element_type=F32
        )

    def add(t, term):
        slot = (index[t] >> 8) & 255
        acc[slot] = acc[slot] + term

    over_tiles(index[slots], tiles, buf, sems, prepare, product, add)
    for s in range(out.shape[0] - 1):
        out[s] = acc[s].T.astype(BF)


SMEM = pl.BlockSpec(memory_space=pltpu.SMEM)
VMEM = pl.BlockSpec(memory_space=pltpu.VMEM)
HBM = pl.BlockSpec(memory_space=pl.ANY)
PARAMS = pltpu.CompilerParams(vmem_limit_bytes=48 * 2**20)


def authority_terms(index, hub, tiles):
    count, side_len, _ = tiles.shape
    vectors = hub.shape[1]
    shape = jax.ShapeDtypeStruct((64, vectors, side_len), BF)
    return pl.pallas_call(
        authority_body,
        name="authority_terms",
        in_specs=[SMEM, VMEM, HBM],
        out_specs=[VMEM, VMEM],
        out_shape=[shape, shape],
        scratch_shapes=[
            pltpu.VMEM(tiles.shape, BF),
            pltpu.VMEM((129, vectors, side_len), F32),
            pltpu.VMEM(hub.shape, BF),
            pltpu.SemaphoreType.DMA((count // PIECE,)),
        ],
        compiler_params=PARAMS,
        cost_estimate=pl.CostEstimate(
            flops=2 * count * vectors * side_len**2, bytes_accessed=tiles.size * 2, transcendentals=0
        ),
    )(index, hub, tiles)


def hub_terms(index, pieces, tiles, slot_count):
    count, side_len, _ = tiles.shape
    vectors = pieces[0].shape[1]
    return pl.pallas_call(
        hub_body,
        name="hub_terms",
        in_specs=[SMEM] + [VMEM] * len(pieces) + [HBM],
        out_specs=VMEM,
        out_shape=jax.ShapeDtypeStruct((slot_count + 1, vectors, side_len), BF),
        scratch_shapes=[
            pltpu.VMEM(tiles.shape, BF),
            pltpu.VMEM((slot_count + 1, side_len, vectors), F32),
            pltpu.VMEM((128, vectors, side_len), BF),
            pltpu.SemaphoreType.DMA((count // PIECE,)),
        ],
        compiler_params=PARAMS,
        cost_estimate=pl.CostEstimate(
            flops=2 * count * vectors * side_len**2, bytes_accessed=tiles.size * 2, transcendentals=0
        ),
    )(index, *pieces, tiles)


def added(a, b):
    return a.astype(F32) + b.astype(F32)


def reduce_over_plane(keep, send):
    mine = added(keep, swap_core(send))
    size = mine.shape[0] // 4
    out = mine.astype(BF)
    got = {k: shift(out[k * size : (k + 1) * size], 0, k).astype(F32) for k in FAR_FIRST}
    mine = (mine[:size] + got[1] + got[2] + got[3]).astype(BF)
    got = {k: shift(mine, 1, k).astype(F32) for k in FAR_FIRST}
    return (mine.astype(F32) + got[2]) + (got[1] + got[3])


def gather_over_ring(mine):
    got = {k: shift(mine, 0, -k) for k in FAR_FIRST}
    half = [mine, got[1], got[2], got[3]]
    return half + [swap_core(piece) for piece in half]


def sum_over_rows(value):
    size = lax.axis_size("row")
    copies = jnp.broadcast_to(value[None], (size, *value.shape))
    return jnp.sum(lax.all_to_all(copies, "row", 0, 0, tiled=True), axis=0)


def norm_scale(squares, host_count):
    return 1.0 / jnp.sqrt(squares / host_count + 1.0)


def local(hub_seeds, tile_blocks, tile_rows, tile_cols, tile_count, row_blocks):
    own_row = lax.axis_index("row")
    own_col = lax.axis_index("col")
    slot_count = hub_seeds.shape[0]
    tile_slots = tile_blocks.shape[0]
    host_count = RB_DEV * row_blocks.shape[0] * tile_blocks.shape[1]
    ranges = jnp.arange(row_blocks.shape[0], dtype=jnp.int32)
    first_block = jnp.sum(jnp.where(ranges < own_row, row_blocks, 0))
    usable = jnp.sum(jnp.where(ranges == own_row, row_blocks, 0))
    live = jnp.arange(tile_slots, dtype=jnp.int32) < tile_count[0]
    slot = jnp.clip(tile_rows - first_block, 0, slot_count - 1)
    to_slot = jnp.where(live, slot, slot_count)
    where = jnp.where(live, positions(own_row, tile_cols), 128)
    packed = slot + to_slot * 256 + where * 65536
    tail = jnp.zeros((128,), jnp.int32)
    tail = jnp.where(jnp.arange(128) == 0, tile_count[0], tail)
    tail = jnp.where(jnp.arange(128) == 1, own_row, tail)
    tail = jnp.where(jnp.arange(128) == 2, own_col, tail)
    tail = jnp.where(jnp.arange(128) == 3, usable, tail)
    index = jnp.concatenate([packed, tail])
    hub = hub_seeds
    hub_squares = []
    for iteration in range(ITERS):
        keep, send = authority_terms(index, hub, tile_blocks)
        ring = reduce_over_plane(keep, send)
        terms = hub_terms(index, gather_over_ring(ring.astype(BF)), tile_blocks, slot_count)
        terms = added(terms, swap_y(terms, 0)).astype(BF)
        terms = added(terms, swap_y(terms, 1))
        squares = jnp.sum(terms[slot_count], axis=1)
        scale = norm_scale(squares, host_count)
        raw_hub = terms[:slot_count] * scale[None, :, None]
        hub = raw_hub.astype(BF)
        hub_squares.append(jnp.sum(raw_hub * raw_hub, axis=(0, 2)))
    everyone = sum_over_rows(jnp.concatenate(hub_squares))
    vectors = squares.shape[0]
    open_scale = norm_scale(everyone[:vectors], host_count)
    authority_scale = open_scale * norm_scale(open_scale * open_scale * squares, host_count)
    rest = authority_scale / scale
    hub_scale = rest * norm_scale(rest * rest * everyone[vectors:], host_count)
    second = jnp.where((own_row & 1) == 0, (own_row >> 1) & 3, own_row >> 3)
    own = lax.dynamic_slice_in_dim(ring, second * GROUP, GROUP)
    authority = (own * authority_scale[None, :, None]).astype(BF)
    return authority, (raw_hub * hub_scale[None, :, None]).astype(BF)


def solution(mesh):
    both = ("row", "col")
    return jax.shard_map(
        local,
        mesh=mesh,
        in_specs=(P("row"), P(both), P(both), P(both), P(both), P()),
        out_specs=(P(both), P("row")),
        check_vma=False,
    )
```

```python
import jax
import jax.numpy as jnp
from jax import lax
from jax.experimental import pallas as pl
from jax.experimental.pallas import tpu as pltpu
from jax.sharding import PartitionSpec as P

ITERS = 2
RB_DEV = 16
GROUP = 4
FIRST = 32
CHUNK = 92
AHEAD = 3
BF = jnp.bfloat16
F32 = jnp.float32

FAR_FIRST = (2, 1, 3)


def moved(r, step, k):
    x, z, c = r >> 3, (r >> 1) & 3, r & 1
    if (c + step) % 2 == 0:
        x = (x + k) % 4
    else:
        z = (z + k) % 4
    return x * 8 + z * 2 + c


def shift(value, step, k):
    return lax.ppermute(value, "row", [(r, moved(r, step, k)) for r in range(32)])


def swap_core(value):
    return lax.ppermute(value, "row", [(r, r ^ 1) for r in range(32)])


def swap_y(value, step):
    perm = []
    for r in range(32):
        for y in range(4):
            to = y ^ 1 if (r + step) % 2 == 0 else 3 - y
            perm.append((r * 4 + y, r * 4 + to))
    return lax.ppermute(value, ("row", "col"), perm)


def positions(own_row, tile_cols):
    owner = tile_cols // RB_DEV
    core = owner & 1
    at_x, at_z = owner >> 3, (owner >> 1) & 3
    first = jnp.where(core == 0, at_x - (own_row >> 3), at_z - (own_row >> 1)) & 3
    second = jnp.where(core == 0, at_z, at_x)
    return (core ^ (own_row & 1)) * 64 + first * 16 + second * 4 + tile_cols % GROUP


def split_sum(total, lane, first):
    out = jnp.zeros(total.shape[:1] + lane.shape[1:], BF)
    rest = total
    for part in range(3):
        piece = rest.astype(BF)
        rest = rest - piece.astype(F32)
        out = jnp.where(lane == first + part, piece, out)
    return out


def over_tiles(count, tiles, buf, sems, prepare, product, add):
    chunks = (count - FIRST + CHUNK - 1) // CHUNK

    def copy(first, size, sem):
        rows = pl.ds(first, size)
        return pltpu.make_async_copy(tiles.at[rows], buf.at[rows], sems.at[sem])

    def chunk(c):
        return copy(FIRST + c * CHUNK, CHUNK, c + 1)

    copy(0, FIRST, 0).start()
    for c in range(AHEAD):

        @pl.when(c < chunks)
        def _():
            chunk(c).start()

    prepare()

    def run(first, size):
        terms = [product(first + u) for u in range(size)]
        for u in range(size):
            add(first + u, terms[u])

    copy(0, FIRST, 0).wait()
    run(0, FIRST)

    def step(c, carry):
        @pl.when(c + AHEAD < chunks)
        def _():
            chunk(c + AHEAD).start()

        chunk(c).wait()
        run(FIRST + c * CHUNK, CHUNK)
        return carry

    lax.fori_loop(0, chunks, step, 0)


def own_range(row_blocks):
    own_row = lax.axis_index("row")
    first, length = jnp.int32(0), jnp.int32(0)
    for r in range(row_blocks.shape[0]):
        first = first + jnp.where(r < own_row, row_blocks[r], 0)
        length = length + jnp.where(r == own_row, row_blocks[r], 0)
    return first, length


def authority_body(index, count, row_blocks, hub, tiles, keep, send, buf, acc, used, sems):
    first_block, usable = own_range(row_blocks)
    live = count[0]

    def prepare():
        acc[...] = jnp.zeros_like(acc)
        for s in range(hub.shape[0]):
            used[s] = jnp.where(s < usable, hub[s], jnp.zeros_like(hub[s]))

    def product(t):
        slot = jnp.clip((index[t] & 0xFFFF) - first_block, 0, hub.shape[0] - 1)
        return jnp.dot(used[slot], buf[t], preferred_element_type=F32)

    def add(t, term):
        where = jnp.where(t < live, index[t] >> 16, 128)
        acc[where] = acc[where] + term

    over_tiles(live, tiles, buf, sems, prepare, product, add)
    keep[...] = acc[:64].astype(BF)
    send[...] = acc[64:128].astype(BF)


def hub_body(index, count, row_blocks, *refs):
    *pieces, tiles, out, buf, acc, gathered, sems = refs
    first_block, _ = own_range(row_blocks)
    live = count[0]
    size = pieces[0].shape[0]
    slots = out.shape[0] - 1

    def prepare():
        acc[...] = jnp.zeros_like(acc)

        def take(b, squares):
            for q, piece in enumerate(pieces):
                block = piece[b]
                gathered[q * size + b] = block
                values = block.astype(F32)
                squares = squares + values * values
            return squares

        squares = lax.fori_loop(0, size, take, jnp.zeros(pieces[0].shape[1:], F32))
        total = jnp.sum(squares, axis=1, keepdims=True)
        lane = lax.broadcasted_iota(jnp.int32, squares.shape, 1)
        out[slots] = split_sum(total, lane, 3 * lax.axis_index("col"))

    def product(t):
        return lax.dot_general(
            buf[t], gathered[index[t] >> 16], (((1,), (1,)), ((), ())), preferred_element_type=F32
        )

    def add(t, term):
        slot = jnp.clip((index[t] & 0xFFFF) - first_block, 0, slots - 1)
        slot = jnp.where(t < live, slot, slots)
        acc[slot] = acc[slot] + term

    over_tiles(live, tiles, buf, sems, prepare, product, add)
    for s in range(slots):
        out[s] = acc[s].T.astype(BF)


SMEM = pl.BlockSpec(memory_space=pltpu.SMEM)
VMEM = pl.BlockSpec(memory_space=pltpu.VMEM)
HBM = pl.BlockSpec(memory_space=pl.ANY)
PARAMS = pltpu.CompilerParams(vmem_limit_bytes=48 * 2**20)


def authority_terms(lists, hub, tiles):
    count, side_len, _ = tiles.shape
    vectors = hub.shape[1]
    shape = jax.ShapeDtypeStruct((64, vectors, side_len), BF)
    return pl.pallas_call(
        authority_body,
        name="authority_terms",
        in_specs=[SMEM, SMEM, SMEM, VMEM, HBM],
        out_specs=[VMEM, VMEM],
        out_shape=[shape, shape],
        scratch_shapes=[
            pltpu.VMEM(tiles.shape, BF),
            pltpu.VMEM((129, vectors, side_len), F32),
            pltpu.VMEM(hub.shape, BF),
            pltpu.SemaphoreType.DMA(((count - FIRST) // CHUNK + 1,)),
        ],
        compiler_params=PARAMS,
        cost_estimate=pl.CostEstimate(
            flops=2 * count * vectors * side_len**2, bytes_accessed=tiles.size * 2, transcendentals=0
        ),
    )(*lists, hub, tiles)


def hub_terms(lists, pieces, tiles, slot_count):
    count, side_len, _ = tiles.shape
    vectors = pieces[0].shape[1]
    return pl.pallas_call(
        hub_body,
        name="hub_terms",
        in_specs=[SMEM] * 3 + [VMEM] * len(pieces) + [HBM],
        out_specs=VMEM,
        out_shape=jax.ShapeDtypeStruct((slot_count + 1, vectors, side_len), BF),
        scratch_shapes=[
            pltpu.VMEM(tiles.shape, BF),
            pltpu.VMEM((slot_count + 1, side_len, vectors), F32),
            pltpu.VMEM((128, vectors, side_len), BF),
            pltpu.SemaphoreType.DMA(((count - FIRST) // CHUNK + 1,)),
        ],
        compiler_params=PARAMS,
        cost_estimate=pl.CostEstimate(
            flops=2 * count * vectors * side_len**2, bytes_accessed=tiles.size * 2, transcendentals=0
        ),
    )(*lists, *pieces, tiles)


def added(a, b):
    return a.astype(F32) + b.astype(F32)


def reduce_over_plane(keep, send):
    mine = added(keep, swap_core(send))
    size = mine.shape[0] // 4
    out = mine.astype(BF)
    got = {k: shift(out[k * size : (k + 1) * size], 0, k).astype(F32) for k in FAR_FIRST}
    mine = (mine[:size] + got[1] + got[2] + got[3]).astype(BF)
    got = {k: shift(mine, 1, k).astype(F32) for k in FAR_FIRST}
    return (mine.astype(F32) + got[2]) + (got[1] + got[3])


def gather_over_ring(mine):
    got = {k: shift(mine, 0, -k) for k in FAR_FIRST}
    half = [mine, got[1], got[2], got[3]]
    return half + [swap_core(piece) for piece in half]


def sum_over_rows(value):
    size = lax.axis_size("row")
    copies = jnp.broadcast_to(value[None], (size, *value.shape))
    return jnp.sum(lax.all_to_all(copies, "row", 0, 0, tiled=True), axis=0)


def norm_scale(squares, host_count):
    return 1.0 / jnp.sqrt(squares / host_count + 1.0)


def local(hub_seeds, tile_blocks, tile_rows, tile_cols, tile_count, row_blocks):
    own_row = lax.axis_index("row")
    slot_count = hub_seeds.shape[0]
    host_count = RB_DEV * row_blocks.shape[0] * tile_blocks.shape[1]
    lists = (tile_rows + positions(own_row, tile_cols) * 65536, tile_count, row_blocks)
    hub = hub_seeds
    hub_squares = []
    for iteration in range(ITERS):
        keep, send = authority_terms(lists, hub, tile_blocks)
        ring = reduce_over_plane(keep, send)
        terms = hub_terms(lists, gather_over_ring(ring.astype(BF)), tile_blocks, slot_count)
        terms = added(terms, swap_y(terms, 0)).astype(BF)
        terms = added(terms, swap_y(terms, 1))
        squares = jnp.sum(terms[slot_count], axis=1)
        scale = norm_scale(squares, host_count)
        raw_hub = terms[:slot_count] * scale[None, :, None]
        hub = raw_hub.astype(BF)
        hub_squares.append(jnp.sum(raw_hub * raw_hub, axis=(0, 2)))
    everyone = sum_over_rows(jnp.concatenate(hub_squares))
    vectors = squares.shape[0]
    open_scale = norm_scale(everyone[:vectors], host_count)
    authority_scale = open_scale * norm_scale(open_scale * open_scale * squares, host_count)
    rest = authority_scale / scale
    hub_scale = rest * norm_scale(rest * rest * everyone[vectors:], host_count)
    second = jnp.where((own_row & 1) == 0, (own_row >> 1) & 3, own_row >> 3)
    own = lax.dynamic_slice_in_dim(ring, second * GROUP, GROUP)
    authority = (own * authority_scale[None, :, None]).astype(BF)
    return authority, (raw_hub * hub_scale[None, :, None]).astype(BF)


def solution(mesh):
    both = ("row", "col")
    return jax.shard_map(
        local,
        mesh=mesh,
        in_specs=(P("row"), P(both), P(both), P(both), P(both), P()),
        out_specs=(P(both), P("row")),
        check_vma=False,
    )
```

```python
import functools

import jax
import jax.numpy as jnp
from jax import lax
from jax.experimental import pallas as pl
from jax.experimental.pallas import tpu as pltpu
from jax.sharding import PartitionSpec as P

ITERS = 2
RB_DEV = 16
GROUP = 4
LAST = 32
CHUNK = 92
AHEAD = 3
BF = jnp.bfloat16
F32 = jnp.float32

FAR_FIRST = (2, 1, 3)


def moved(r, step, k):
    x, z, c = r >> 3, (r >> 1) & 3, r & 1
    if (c + step) % 2 == 0:
        x = (x + k) % 4
    else:
        z = (z + k) % 4
    return x * 8 + z * 2 + c


def shift(value, step, k):
    return lax.ppermute(value, "row", [(r, moved(r, step, k)) for r in range(32)])


def swap_core(value):
    return lax.ppermute(value, "row", [(r, r ^ 1) for r in range(32)])


def swap_y(value, step):
    perm = []
    for r in range(32):
        for y in range(4):
            to = y ^ 1 if (r + step) % 2 == 0 else 3 - y
            perm.append((r * 4 + y, r * 4 + to))
    return lax.ppermute(value, ("row", "col"), perm)


def positions(own_row, tile_cols):
    owner = tile_cols // RB_DEV
    core = owner & 1
    at_x, at_z = owner >> 3, (owner >> 1) & 3
    first = jnp.where(core == 0, at_x - (own_row >> 3), at_z - (own_row >> 1)) & 3
    second = jnp.where(core == 0, at_z, at_x)
    return (core ^ (own_row & 1)) * 64 + first * 16 + second * 4 + tile_cols % GROUP


def split_sum(total, lane, first):
    out = jnp.zeros(total.shape[:1] + lane.shape[1:], BF)
    rest = total
    for part in range(3):
        piece = rest.astype(BF)
        rest = rest - piece.astype(F32)
        out = jnp.where(lane == first + part, piece, out)
    return out


def over_tiles(count, tiles, buf, sems, prepare, product, add):
    full = tiles.shape[0] // CHUNK
    last = full * CHUNK
    chunks = jnp.minimum((count + CHUNK - 1) // CHUNK, full)

    def copy(first, size, sem):
        rows = pl.ds(first, size)
        return pltpu.make_async_copy(tiles.at[rows], buf.at[rows], sems.at[sem])

    def chunk(c):
        return copy(c * CHUNK, CHUNK, c)

    for c in range(AHEAD):

        @pl.when(c < chunks)
        def _():
            chunk(c).start()

    prepare()

    def run(first, size):
        terms = [product(first + u) for u in range(size)]
        for u in range(size):
            add(first + u, terms[u])

    def step(c, carry):
        @pl.when(c + AHEAD < chunks)
        def _():
            chunk(c + AHEAD).start()

        @pl.when(jnp.logical_and(c + AHEAD == full, count > last))
        def _():
            copy(last, LAST, full).start()

        chunk(c).wait()
        run(c * CHUNK, CHUNK)
        return carry

    lax.fori_loop(0, chunks, step, 0)

    @pl.when(count > last)
    def _():
        copy(last, LAST, full).wait()
        run(last, LAST)


def own_range(row_blocks):
    own_row = lax.axis_index("row")
    first, length = jnp.int32(0), jnp.int32(0)
    for r in range(row_blocks.shape[0]):
        first = first + jnp.where(r < own_row, row_blocks[r], 0)
        length = length + jnp.where(r == own_row, row_blocks[r], 0)
    return first, length


def authority_body(
    index, count, row_blocks, hub, tiles, keep, send, buf, acc, used, sems, *, from_hbm
):
    first_block, usable = own_range(row_blocks)
    live = count[0]
    source = hub
    if from_hbm:
        seeds = pltpu.make_async_copy(hub, used, sems.at[sems.shape[0] - 1])
        seeds.start()
        source = used

    def prepare():
        acc[...] = jnp.zeros_like(acc)
        if from_hbm:
            seeds.wait()
        for s in range(hub.shape[0]):
            block = source[s]
            used[s] = jnp.where(s < usable, block, jnp.zeros_like(block))

    def product(t):
        slot = jnp.clip((index[t] & 0xFFFF) - first_block, 0, hub.shape[0] - 1)
        return jnp.dot(used[slot], buf[t], preferred_element_type=F32)

    def add(t, term):
        where = jnp.where(t < live, index[t] >> 16, 128)
        acc[where] = acc[where] + term

    over_tiles(live, tiles, buf, sems, prepare, product, add)
    keep[...] = acc[:64].astype(BF)
    send[...] = acc[64:128].astype(BF)


def hub_body(index, count, row_blocks, *refs):
    *pieces, tiles, out, buf, acc, gathered, sems = refs
    first_block, _ = own_range(row_blocks)
    live = count[0]
    size = pieces[0].shape[0]
    slots = out.shape[0] - 1

    def prepare():
        acc[...] = jnp.zeros_like(acc)

        def take(b, squares):
            for q, piece in enumerate(pieces):
                block = piece[b]
                gathered[q * size + b] = block
                values = block.astype(F32)
                squares = squares + values * values
            return squares

        squares = lax.fori_loop(0, size, take, jnp.zeros(pieces[0].shape[1:], F32))
        total = jnp.sum(squares, axis=1, keepdims=True)
        lane = lax.broadcasted_iota(jnp.int32, squares.shape, 1)
        out[slots] = split_sum(total, lane, 3 * lax.axis_index("col"))

    def product(t):
        return lax.dot_general(
            buf[t], gathered[index[t] >> 16], (((1,), (1,)), ((), ())), preferred_element_type=F32
        )

    def add(t, term):
        slot = jnp.clip((index[t] & 0xFFFF) - first_block, 0, slots - 1)
        slot = jnp.where(t < live, slot, slots)
        acc[slot] = acc[slot] + term

    over_tiles(live, tiles, buf, sems, prepare, product, add)
    for s in range(slots):
        out[s] = acc[s].T.astype(BF)


SMEM = pl.BlockSpec(memory_space=pltpu.SMEM)
VMEM = pl.BlockSpec(memory_space=pltpu.VMEM)
HBM = pl.BlockSpec(memory_space=pl.ANY)
PARAMS = pltpu.CompilerParams(vmem_limit_bytes=48 * 2**20)


def authority_terms(lists, hub, tiles, from_hbm):
    count, side_len, _ = tiles.shape
    vectors = hub.shape[1]
    shape = jax.ShapeDtypeStruct((64, vectors, side_len), BF)
    return pl.pallas_call(
        functools.partial(authority_body, from_hbm=from_hbm),
        name="authority_terms",
        in_specs=[SMEM, SMEM, SMEM, HBM if from_hbm else VMEM, HBM],
        out_specs=[VMEM, VMEM],
        out_shape=[shape, shape],
        scratch_shapes=[
            pltpu.VMEM(tiles.shape, BF),
            pltpu.VMEM((129, vectors, side_len), F32),
            pltpu.VMEM(hub.shape, BF),
            pltpu.SemaphoreType.DMA((count // CHUNK + 2,)),
        ],
        compiler_params=PARAMS,
        cost_estimate=pl.CostEstimate(
            flops=2 * count * vectors * side_len**2, bytes_accessed=tiles.size * 2, transcendentals=0
        ),
    )(*lists, hub, tiles)


def hub_terms(lists, pieces, tiles, slot_count):
    count, side_len, _ = tiles.shape
    vectors = pieces[0].shape[1]
    return pl.pallas_call(
        hub_body,
        name="hub_terms",
        in_specs=[SMEM] * 3 + [VMEM] * len(pieces) + [HBM],
        out_specs=VMEM,
        out_shape=jax.ShapeDtypeStruct((slot_count + 1, vectors, side_len), BF),
        scratch_shapes=[
            pltpu.VMEM(tiles.shape, BF),
            pltpu.VMEM((slot_count + 1, side_len, vectors), F32),
            pltpu.VMEM((128, vectors, side_len), BF),
            pltpu.SemaphoreType.DMA((count // CHUNK + 2,)),
        ],
        compiler_params=PARAMS,
        cost_estimate=pl.CostEstimate(
            flops=2 * count * vectors * side_len**2, bytes_accessed=tiles.size * 2, transcendentals=0
        ),
    )(*lists, *pieces, tiles)


def added(a, b):
    return a.astype(F32) + b.astype(F32)


def reduce_over_plane(keep, send):
    mine = added(keep, swap_core(send))
    size = mine.shape[0] // 4
    out = mine.astype(BF)
    got = {k: shift(out[k * size : (k + 1) * size], 0, k).astype(F32) for k in FAR_FIRST}
    mine = (mine[:size] + got[1] + got[2] + got[3]).astype(BF)
    got = {k: shift(mine, 1, k).astype(F32) for k in FAR_FIRST}
    return (mine.astype(F32) + got[2]) + (got[1] + got[3])


def gather_over_ring(mine):
    got = {k: shift(mine, 0, -k) for k in FAR_FIRST}
    half = [mine, got[1], got[2], got[3]]
    return half + [swap_core(piece) for piece in half]


def sum_over_rows(value):
    size = lax.axis_size("row")
    copies = jnp.broadcast_to(value[None], (size, *value.shape))
    return jnp.sum(lax.all_to_all(copies, "row", 0, 0, tiled=True), axis=0)


def norm_scale(squares, host_count):
    return 1.0 / jnp.sqrt(squares / host_count + 1.0)


def local(hub_seeds, tile_blocks, tile_rows, tile_cols, tile_count, row_blocks):
    own_row = lax.axis_index("row")
    slot_count = hub_seeds.shape[0]
    host_count = RB_DEV * row_blocks.shape[0] * tile_blocks.shape[1]
    lists = (tile_rows + positions(own_row, tile_cols) * 65536, tile_count, row_blocks)
    hub = hub_seeds
    hub_squares = []
    for iteration in range(ITERS):
        keep, send = authority_terms(lists, hub, tile_blocks, iteration == 0)
        ring = reduce_over_plane(keep, send)
        terms = hub_terms(lists, gather_over_ring(ring.astype(BF)), tile_blocks, slot_count)
        terms = added(terms, swap_y(terms, 0)).astype(BF)
        terms = added(terms, swap_y(terms, 1))
        squares = jnp.sum(terms[slot_count], axis=1)
        scale = norm_scale(squares, host_count)
        raw_hub = terms[:slot_count] * scale[None, :, None]
        hub = raw_hub.astype(BF)
        hub_squares.append(jnp.sum(raw_hub * raw_hub, axis=(0, 2)))
    everyone = sum_over_rows(jnp.concatenate(hub_squares))
    vectors = squares.shape[0]
    open_scale = norm_scale(everyone[:vectors], host_count)
    authority_scale = open_scale * norm_scale(open_scale * open_scale * squares, host_count)
    rest = authority_scale / scale
    hub_scale = rest * norm_scale(rest * rest * everyone[vectors:], host_count)
    second = jnp.where((own_row & 1) == 0, (own_row >> 1) & 3, own_row >> 3)
    own = lax.dynamic_slice_in_dim(ring, second * GROUP, GROUP)
    authority = (own * authority_scale[None, :, None]).astype(BF)
    return authority, (raw_hub * hub_scale[None, :, None]).astype(BF)


def solution(mesh):
    both = ("row", "col")
    return jax.shard_map(
        local,
        mesh=mesh,
        in_specs=(P("row"), P(both), P(both), P(both), P(both), P()),
        out_specs=(P(both), P("row")),
        check_vma=False,
    )
```

```python
import functools

import jax
import jax.numpy as jnp
from jax import lax
from jax.experimental import pallas as pl
from jax.experimental.pallas import tpu as pltpu
from jax.sharding import PartitionSpec as P

ITERS = 2
RB_DEV = 16
GROUP = 4
LAST = 32
CHUNK = 92
AHEAD = 3
BF = jnp.bfloat16
F32 = jnp.float32

FAR_FIRST = (2, 1, 3)


def moved(r, step, k):
    x, z, c = r >> 3, (r >> 1) & 3, r & 1
    if (c + step) % 2 == 0:
        x = (x + k) % 4
    else:
        z = (z + k) % 4
    return x * 8 + z * 2 + c


def shift(value, step, k):
    return lax.ppermute(value, "row", [(r, moved(r, step, k)) for r in range(32)])


def swap_core(value):
    return lax.ppermute(value, "row", [(r, r ^ 1) for r in range(32)])


def swap_y(value, step):
    perm = []
    for r in range(32):
        for y in range(4):
            to = y ^ 1 if (r + step) % 2 == 0 else 3 - y
            perm.append((r * 4 + y, r * 4 + to))
    return lax.ppermute(value, ("row", "col"), perm)


def positions(own_row, tile_cols):
    owner = tile_cols // RB_DEV
    core = owner & 1
    at_x, at_z = owner >> 3, (owner >> 1) & 3
    first = jnp.where(core == 0, at_x - (own_row >> 3), at_z - (own_row >> 1)) & 3
    second = jnp.where(core == 0, at_z, at_x)
    return (core ^ (own_row & 1)) * 64 + first * 16 + second * 4 + tile_cols % GROUP


def split_sum(total, lane, first):
    out = jnp.zeros(total.shape[:1] + lane.shape[1:], BF)
    rest = total
    for part in range(3):
        piece = rest.astype(BF)
        rest = rest - piece.astype(F32)
        out = jnp.where(lane == first + part, piece, out)
    return out


def over_tiles(count, tiles, buf, sems, prepare, product, add):
    full = tiles.shape[0] // CHUNK
    last = full * CHUNK
    chunks = jnp.minimum((count + CHUNK - 1) // CHUNK, full)

    def copy(first, size, sem):
        rows = pl.ds(first, size)
        return pltpu.make_async_copy(tiles.at[rows], buf.at[rows], sems.at[sem])

    def chunk(c):
        return copy(c * CHUNK, CHUNK, c)

    for c in range(AHEAD):

        @pl.when(c < chunks)
        def _():
            chunk(c).start()

    prepare()

    def run(first, size):
        terms = [product(first + u) for u in range(size)]
        for u in range(size):
            add(first + u, terms[u])

    def step(c, carry):
        @pl.when(c + AHEAD < chunks)
        def _():
            chunk(c + AHEAD).start()

        @pl.when(jnp.logical_and(c + AHEAD == full, count > last))
        def _():
            copy(last, LAST, full).start()

        chunk(c).wait()
        run(c * CHUNK, CHUNK)
        return carry

    lax.fori_loop(0, chunks, step, 0)

    @pl.when(count > last)
    def _():
        copy(last, LAST, full).wait()
        run(last, LAST)


def own_range(row_blocks, lengths, sem):
    copy = pltpu.make_async_copy(row_blocks, lengths, sem)
    copy.start()
    copy.wait()
    own_row = lax.axis_index("row")
    first, length = jnp.int32(0), jnp.int32(0)
    for r in range(row_blocks.shape[0]):
        first = first + jnp.where(r < own_row, lengths[r], 0)
        length = length + jnp.where(r == own_row, lengths[r], 0)
    return first, length


def authority_body(
    index, count, row_blocks, hub, tiles, keep, send, buf, acc, used, lengths, sems, *, from_hbm
):
    live = count[0]
    source = hub
    if from_hbm:
        seeds = pltpu.make_async_copy(hub, used, sems.at[sems.shape[0] - 1])
        seeds.start()
        source = used
    where_from = {}

    def prepare():
        first_block, usable = own_range(row_blocks, lengths, sems.at[sems.shape[0] - 2])
        where_from[0] = first_block
        acc[...] = jnp.zeros_like(acc)
        if from_hbm:
            seeds.wait()
        for s in range(hub.shape[0]):
            block = source[s]
            used[s] = jnp.where(s < usable, block, jnp.zeros_like(block))

    def product(t):
        slot = jnp.clip((index[t] & 0xFFFF) - where_from[0], 0, hub.shape[0] - 1)
        return jnp.dot(used[slot], buf[t], preferred_element_type=F32)

    def add(t, term):
        where = jnp.where(t < live, index[t] >> 16, 128)
        acc[where] = acc[where] + term

    over_tiles(live, tiles, buf, sems, prepare, product, add)
    keep[...] = acc[:64].astype(BF)
    send[...] = acc[64:128].astype(BF)


def hub_body(index, count, row_blocks, *refs):
    *pieces, tiles, out, buf, acc, gathered, lengths, sems = refs
    live = count[0]
    where_from = {}
    size = pieces[0].shape[0]
    slots = out.shape[0] - 1

    def prepare():
        where_from[0], _ = own_range(row_blocks, lengths, sems.at[sems.shape[0] - 2])
        acc[...] = jnp.zeros_like(acc)

        def take(b, squares):
            for q, piece in enumerate(pieces):
                block = piece[b]
                gathered[q * size + b] = block
                values = block.astype(F32)
                squares = squares + values * values
            return squares

        squares = lax.fori_loop(0, size, take, jnp.zeros(pieces[0].shape[1:], F32))
        total = jnp.sum(squares, axis=1, keepdims=True)
        lane = lax.broadcasted_iota(jnp.int32, squares.shape, 1)
        out[slots] = split_sum(total, lane, 3 * lax.axis_index("col"))

    def product(t):
        return lax.dot_general(
            buf[t], gathered[index[t] >> 16], (((1,), (1,)), ((), ())), preferred_element_type=F32
        )

    def add(t, term):
        slot = jnp.clip((index[t] & 0xFFFF) - where_from[0], 0, slots - 1)
        slot = jnp.where(t < live, slot, slots)
        acc[slot] = acc[slot] + term

    over_tiles(live, tiles, buf, sems, prepare, product, add)
    for s in range(slots):
        out[s] = acc[s].T.astype(BF)


SMEM = pl.BlockSpec(memory_space=pltpu.SMEM)
VMEM = pl.BlockSpec(memory_space=pltpu.VMEM)
HBM = pl.BlockSpec(memory_space=pltpu.HBM)
PARAMS = pltpu.CompilerParams(vmem_limit_bytes=48 * 2**20)


def authority_terms(lists, hub, tiles, from_hbm):
    count, side_len, _ = tiles.shape
    vectors = hub.shape[1]
    shape = jax.ShapeDtypeStruct((64, vectors, side_len), BF)
    return pl.pallas_call(
        functools.partial(authority_body, from_hbm=from_hbm),
        name="authority_terms",
        in_specs=[SMEM, SMEM, HBM, HBM if from_hbm else VMEM, HBM],
        out_specs=[VMEM, VMEM],
        out_shape=[shape, shape],
        scratch_shapes=[
            pltpu.VMEM(tiles.shape, BF),
            pltpu.VMEM((129, vectors, side_len), F32),
            pltpu.VMEM(hub.shape, BF),
            pltpu.SMEM(lists[2].shape, jnp.int32),
            pltpu.SemaphoreType.DMA((count // CHUNK + 3,)),
        ],
        compiler_params=PARAMS,
        cost_estimate=pl.CostEstimate(
            flops=2 * count * vectors * side_len**2, bytes_accessed=tiles.size * 2, transcendentals=0
        ),
    )(*lists, hub, tiles)


def hub_terms(lists, pieces, tiles, slot_count):
    count, side_len, _ = tiles.shape
    vectors = pieces[0].shape[1]
    return pl.pallas_call(
        hub_body,
        name="hub_terms",
        in_specs=[SMEM, SMEM, HBM] + [VMEM] * len(pieces) + [HBM],
        out_specs=VMEM,
        out_shape=jax.ShapeDtypeStruct((slot_count + 1, vectors, side_len), BF),
        scratch_shapes=[
            pltpu.VMEM(tiles.shape, BF),
            pltpu.VMEM((slot_count + 1, side_len, vectors), F32),
            pltpu.VMEM((128, vectors, side_len), BF),
            pltpu.SMEM(lists[2].shape, jnp.int32),
            pltpu.SemaphoreType.DMA((count // CHUNK + 3,)),
        ],
        compiler_params=PARAMS,
        cost_estimate=pl.CostEstimate(
            flops=2 * count * vectors * side_len**2, bytes_accessed=tiles.size * 2, transcendentals=0
        ),
    )(*lists, *pieces, tiles)


def added(a, b):
    return a.astype(F32) + b.astype(F32)


def reduce_over_plane(keep, send):
    got = swap_core(send)
    both = [added(part, other) for part, other in zip(jnp.split(keep, 4), jnp.split(got, 4))]
    got = {k: shift(both[k].astype(BF), 0, k).astype(F32) for k in FAR_FIRST}
    mine = (both[0] + got[1] + got[2] + got[3]).astype(BF)
    got = {k: shift(mine, 1, k).astype(F32) for k in FAR_FIRST}
    return (mine.astype(F32) + got[2]) + (got[1] + got[3])


def gather_over_ring(mine):
    got = {k: shift(mine, 0, -k) for k in FAR_FIRST}
    half = [mine, got[1], got[2], got[3]]
    return half + [swap_core(piece) for piece in half]


def sum_over_rows(value):
    size = lax.axis_size("row")
    copies = jnp.broadcast_to(value[None], (size, *value.shape))
    return jnp.sum(lax.all_to_all(copies, "row", 0, 0, tiled=True), axis=0)


def norm_scale(squares, host_count):
    return 1.0 / jnp.sqrt(squares / host_count + 1.0)


def local(hub_seeds, tile_blocks, tile_rows, tile_cols, tile_count, row_blocks):
    own_row = lax.axis_index("row")
    slot_count = hub_seeds.shape[0]
    host_count = RB_DEV * row_blocks.shape[0] * tile_blocks.shape[1]
    lengths = pltpu.with_memory_space_constraint(row_blocks, pltpu.HBM)
    lists = (tile_rows + positions(own_row, tile_cols) * 65536, tile_count, lengths)
    hub = pltpu.with_memory_space_constraint(hub_seeds, pltpu.HBM)
    hub_squares = []
    for iteration in range(ITERS):
        keep, send = authority_terms(lists, hub, tile_blocks, iteration == 0)
        ring = reduce_over_plane(keep, send)
        terms = hub_terms(lists, gather_over_ring(ring.astype(BF)), tile_blocks, slot_count)
        terms = added(terms, swap_y(terms, 0)).astype(BF)
        terms = added(terms, swap_y(terms, 1))
        squares = jnp.sum(terms[slot_count], axis=1)
        scale = norm_scale(squares, host_count)
        raw_hub = terms[:slot_count] * scale[None, :, None]
        hub = raw_hub.astype(BF)
        hub_squares.append(jnp.sum(raw_hub * raw_hub, axis=(0, 2)))
    everyone = sum_over_rows(jnp.concatenate(hub_squares))
    vectors = squares.shape[0]
    open_scale = norm_scale(everyone[:vectors], host_count)
    authority_scale = open_scale * norm_scale(open_scale * open_scale * squares, host_count)
    rest = authority_scale / scale
    hub_scale = rest * norm_scale(rest * rest * everyone[vectors:], host_count)
    second = jnp.where((own_row & 1) == 0, (own_row >> 1) & 3, own_row >> 3)
    own = lax.dynamic_slice_in_dim(ring, second * GROUP, GROUP)
    authority = (own * authority_scale[None, :, None]).astype(BF)
    return authority, (raw_hub * hub_scale[None, :, None]).astype(BF)


def solution(mesh):
    both = ("row", "col")
    return jax.shard_map(
        local,
        mesh=mesh,
        in_specs=(P("row"), P(both), P(both), P(both), P(both), P()),
        out_specs=(P(both), P("row")),
        check_vma=False,
    )
```

```python
import functools

import jax
import jax.numpy as jnp
from jax import lax
from jax.experimental import pallas as pl
from jax.experimental.pallas import tpu as pltpu
from jax.sharding import PartitionSpec as P

ITERS = 2
RB_DEV = 16
GROUP = 4
LAST = 32
CHUNK = 92
AHEAD = 4
PARTS = 2
BF = jnp.bfloat16
F32 = jnp.float32

FAR_FIRST = (2, 1, 3)


def moved(r, step, k):
    x, z, c = r >> 3, (r >> 1) & 3, r & 1
    if (c + step) % 2 == 0:
        x = (x + k) % 4
    else:
        z = (z + k) % 4
    return x * 8 + z * 2 + c


def shift(value, step, k):
    return lax.ppermute(value, "row", [(r, moved(r, step, k)) for r in range(32)])


def swap_core(value):
    return lax.ppermute(value, "row", [(r, r ^ 1) for r in range(32)])


def swap_y(value, step):
    perm = []
    for r in range(32):
        for y in range(4):
            to = y ^ 1 if (r + step) % 2 == 0 else 3 - y
            perm.append((r * 4 + y, r * 4 + to))
    return lax.ppermute(value, ("row", "col"), perm)


def positions(own_row, tile_cols):
    owner = tile_cols // RB_DEV
    core = owner & 1
    at_x, at_z = owner >> 3, (owner >> 1) & 3
    first = jnp.where(core == 0, at_x - (own_row >> 3), at_z - (own_row >> 1)) & 3
    second = jnp.where(core == 0, at_z, at_x)
    return (core ^ (own_row & 1)) * 64 + first * 16 + second * 4 + tile_cols % GROUP


def split_sum(total, lane, first):
    out = jnp.zeros(total.shape[:1] + lane.shape[1:], BF)
    rest = total
    for part in range(3):
        piece = rest.astype(BF)
        rest = rest - piece.astype(F32)
        out = jnp.where(lane == first + part, piece, out)
    return out


def over_tiles(count, tiles, buf, sems, prepare, product, add):
    full = tiles.shape[0] // CHUNK
    last = full * CHUNK
    chunks = jnp.minimum((count + CHUNK - 1) // CHUNK, full)

    def copy(first, size, sem):
        rows = pl.ds(first, size)
        return pltpu.make_async_copy(tiles.at[rows], buf.at[rows], sems.at[sem])

    def chunk(c):
        return copy(c * CHUNK, CHUNK, c)

    def start_chunk(c):
        for part in range(PARTS):
            copy(c * CHUNK + part * (CHUNK // PARTS), CHUNK // PARTS, c).start()

    for c in range(AHEAD):

        @pl.when(c < chunks)
        def _():
            start_chunk(c)

    prepare()

    def run(first, size):
        terms = [product(first + u) for u in range(size)]
        for u in range(size):
            add(first + u, terms[u])

    def step(c, carry):
        @pl.when(c + AHEAD < chunks)
        def _():
            start_chunk(c + AHEAD)

        @pl.when(jnp.logical_and(c + AHEAD == full, count > last))
        def _():
            copy(last, LAST, full).start()

        chunk(c).wait()
        run(c * CHUNK, CHUNK)
        return carry

    lax.fori_loop(0, chunks, step, 0)

    @pl.when(count > last)
    def _():
        copy(last, LAST, full).wait()
        run(last, LAST)


def own_range(row_blocks, lengths, sem):
    copy = pltpu.make_async_copy(row_blocks, lengths, sem)
    copy.start()
    copy.wait()
    own_row = lax.axis_index("row")
    first, length = jnp.int32(0), jnp.int32(0)
    for r in range(row_blocks.shape[0]):
        first = first + jnp.where(r < own_row, lengths[r], 0)
        length = length + jnp.where(r == own_row, lengths[r], 0)
    return first, length


def authority_body(
    index, count, row_blocks, hub, tiles, keep, send, buf, acc, used, lengths, sems, *, from_hbm
):
    live = count[0]
    source = hub
    if from_hbm:
        seeds = pltpu.make_async_copy(hub, used, sems.at[sems.shape[0] - 1])
        seeds.start()
        source = used
    where_from = {}

    def prepare():
        first_block, usable = own_range(row_blocks, lengths, sems.at[sems.shape[0] - 2])
        where_from[0] = first_block
        acc[...] = jnp.zeros_like(acc)
        if from_hbm:
            seeds.wait()
        for s in range(hub.shape[0]):
            block = source[s]
            used[s] = jnp.where(s < usable, block, jnp.zeros_like(block))

    def product(t):
        slot = jnp.clip((index[t] & 0xFFFF) - where_from[0], 0, hub.shape[0] - 1)
        return jnp.dot(used[slot], buf[t], preferred_element_type=F32)

    def add(t, term):
        where = jnp.where(t < live, index[t] >> 16, 128)
        acc[where] = acc[where] + term

    over_tiles(live, tiles, buf, sems, prepare, product, add)
    keep[...] = acc[:64].astype(BF)
    send[...] = acc[64:128].astype(BF)


def hub_body(index, count, row_blocks, *refs):
    *pieces, tiles, out, buf, acc, gathered, lengths, sems = refs
    live = count[0]
    where_from = {}
    size = pieces[0].shape[0]
    slots = out.shape[0] - 1

    def prepare():
        where_from[0], _ = own_range(row_blocks, lengths, sems.at[sems.shape[0] - 2])
        acc[...] = jnp.zeros_like(acc)

        def take(b, squares):
            for q, piece in enumerate(pieces):
                block = piece[b]
                gathered[q * size + b] = block
                values = block.astype(F32)
                squares = squares + values * values
            return squares

        squares = lax.fori_loop(0, size, take, jnp.zeros(pieces[0].shape[1:], F32))
        total = jnp.sum(squares, axis=1, keepdims=True)
        lane = lax.broadcasted_iota(jnp.int32, squares.shape, 1)
        out[slots] = split_sum(total, lane, 3 * lax.axis_index("col"))

    def product(t):
        return lax.dot_general(
            buf[t], gathered[index[t] >> 16], (((1,), (1,)), ((), ())), preferred_element_type=F32
        )

    def add(t, term):
        slot = jnp.clip((index[t] & 0xFFFF) - where_from[0], 0, slots - 1)
        slot = jnp.where(t < live, slot, slots)
        acc[slot] = acc[slot] + term

    over_tiles(live, tiles, buf, sems, prepare, product, add)
    for s in range(slots):
        out[s] = acc[s].T.astype(BF)


SMEM = pl.BlockSpec(memory_space=pltpu.SMEM)
VMEM = pl.BlockSpec(memory_space=pltpu.VMEM)
HBM = pl.BlockSpec(memory_space=pltpu.HBM)
PARAMS = pltpu.CompilerParams(vmem_limit_bytes=48 * 2**20)


def authority_terms(lists, hub, tiles, from_hbm):
    count, side_len, _ = tiles.shape
    vectors = hub.shape[1]
    shape = jax.ShapeDtypeStruct((64, vectors, side_len), BF)
    return pl.pallas_call(
        functools.partial(authority_body, from_hbm=from_hbm),
        name="authority_terms",
        in_specs=[SMEM, SMEM, HBM, HBM if from_hbm else VMEM, HBM],
        out_specs=[VMEM, VMEM],
        out_shape=[shape, shape],
        scratch_shapes=[
            pltpu.VMEM(tiles.shape, BF),
            pltpu.VMEM((129, vectors, side_len), F32),
            pltpu.VMEM(hub.shape, BF),
            pltpu.SMEM(lists[2].shape, jnp.int32),
            pltpu.SemaphoreType.DMA((count // CHUNK + 3,)),
        ],
        compiler_params=PARAMS,
        cost_estimate=pl.CostEstimate(
            flops=2 * count * vectors * side_len**2, bytes_accessed=tiles.size * 2, transcendentals=0
        ),
    )(*lists, hub, tiles)


def hub_terms(lists, pieces, tiles, slot_count):
    count, side_len, _ = tiles.shape
    vectors = pieces[0].shape[1]
    return pl.pallas_call(
        hub_body,
        name="hub_terms",
        in_specs=[SMEM, SMEM, HBM] + [VMEM] * len(pieces) + [HBM],
        out_specs=VMEM,
        out_shape=jax.ShapeDtypeStruct((slot_count + 1, vectors, side_len), BF),
        scratch_shapes=[
            pltpu.VMEM(tiles.shape, BF),
            pltpu.VMEM((slot_count + 1, side_len, vectors), F32),
            pltpu.VMEM((128, vectors, side_len), BF),
            pltpu.SMEM(lists[2].shape, jnp.int32),
            pltpu.SemaphoreType.DMA((count // CHUNK + 3,)),
        ],
        compiler_params=PARAMS,
        cost_estimate=pl.CostEstimate(
            flops=2 * count * vectors * side_len**2, bytes_accessed=tiles.size * 2, transcendentals=0
        ),
    )(*lists, *pieces, tiles)


def added(a, b):
    return a.astype(F32) + b.astype(F32)


def reduce_over_plane(keep, send):
    got = swap_core(send)
    both = [added(part, other) for part, other in zip(jnp.split(keep, 4), jnp.split(got, 4))]
    got = {k: shift(both[k].astype(BF), 0, k).astype(F32) for k in FAR_FIRST}
    mine = (both[0] + got[1] + got[2] + got[3]).astype(BF)
    got = {k: shift(mine, 1, k).astype(F32) for k in FAR_FIRST}
    return (mine.astype(F32) + got[2]) + (got[1] + got[3])


def gather_over_ring(mine):
    got = {k: shift(mine, 0, -k) for k in FAR_FIRST}
    half = [mine, got[1], got[2], got[3]]
    return half + [swap_core(piece) for piece in half]


def sum_over_rows(value):
    size = lax.axis_size("row")
    copies = jnp.broadcast_to(value[None], (size, *value.shape))
    return jnp.sum(lax.all_to_all(copies, "row", 0, 0, tiled=True), axis=0)


def norm_scale(squares, host_count):
    return 1.0 / jnp.sqrt(squares / host_count + 1.0)


def local(hub_seeds, tile_blocks, tile_rows, tile_cols, tile_count, row_blocks):
    own_row = lax.axis_index("row")
    slot_count = hub_seeds.shape[0]
    host_count = RB_DEV * row_blocks.shape[0] * tile_blocks.shape[1]
    lengths = pltpu.with_memory_space_constraint(row_blocks, pltpu.HBM)
    lists = (tile_rows + positions(own_row, tile_cols) * 65536, tile_count, lengths)
    hub = pltpu.with_memory_space_constraint(hub_seeds, pltpu.HBM)
    hub_squares = []
    for iteration in range(ITERS):
        keep, send = authority_terms(lists, hub, tile_blocks, iteration == 0)
        ring = reduce_over_plane(keep, send)
        terms = hub_terms(lists, gather_over_ring(ring.astype(BF)), tile_blocks, slot_count)
        terms = added(terms, swap_y(terms, 0)).astype(BF)
        terms = added(terms, swap_y(terms, 1))
        squares = jnp.sum(terms[slot_count], axis=1)
        scale = norm_scale(squares, host_count)
        raw_hub = terms[:slot_count] * scale[None, :, None]
        hub = raw_hub.astype(BF)
        hub_squares.append(jnp.sum(raw_hub * raw_hub, axis=(0, 2)))
    everyone = sum_over_rows(jnp.concatenate(hub_squares))
    vectors = squares.shape[0]
    open_scale = norm_scale(everyone[:vectors], host_count)
    authority_scale = open_scale * norm_scale(open_scale * open_scale * squares, host_count)
    rest = authority_scale / scale
    hub_scale = rest * norm_scale(rest * rest * everyone[vectors:], host_count)
    second = jnp.where((own_row & 1) == 0, (own_row >> 1) & 3, own_row >> 3)
    own = lax.dynamic_slice_in_dim(ring, second * GROUP, GROUP)
    authority = (own * authority_scale[None, :, None]).astype(BF)
    return authority, (raw_hub * hub_scale[None, :, None]).astype(BF)


def solution(mesh):
    both = ("row", "col")
    return jax.shard_map(
        local,
        mesh=mesh,
        in_specs=(P("row"), P(both), P(both), P(both), P(both), P()),
        out_specs=(P(both), P("row")),
        check_vma=False,
    )
```

```python
import functools

import jax
import jax.numpy as jnp
from jax import lax
from jax.experimental import pallas as pl
from jax.experimental.pallas import tpu as pltpu
from jax.sharding import PartitionSpec as P

ITERS = 2
RB_DEV = 16
GROUP = 4
LAST = 32
CHUNK = 92
AHEAD = 6
PARTS = 2
BF = jnp.bfloat16
F32 = jnp.float32

FAR_FIRST = (2, 1, 3)


def moved(r, step, k):
    x, z, c = r >> 3, (r >> 1) & 3, r & 1
    if (c + step) % 2 == 0:
        x = (x + k) % 4
    else:
        z = (z + k) % 4
    return x * 8 + z * 2 + c


def shift(value, step, k):
    return lax.ppermute(value, "row", [(r, moved(r, step, k)) for r in range(32)])


def swap_core(value):
    return lax.ppermute(value, "row", [(r, r ^ 1) for r in range(32)])


def swap_y(value, step):
    perm = []
    for r in range(32):
        for y in range(4):
            to = y ^ 1 if (r + step) % 2 == 0 else 3 - y
            perm.append((r * 4 + y, r * 4 + to))
    return lax.ppermute(value, ("row", "col"), perm)


def positions(own_row, tile_cols):
    owner = tile_cols // RB_DEV
    core = owner & 1
    at_x, at_z = owner >> 3, (owner >> 1) & 3
    first = jnp.where(core == 0, at_x - (own_row >> 3), at_z - (own_row >> 1)) & 3
    second = jnp.where(core == 0, at_z, at_x)
    return (core ^ (own_row & 1)) * 64 + first * 16 + second * 4 + tile_cols % GROUP


def split_sum(total, lane, first):
    out = jnp.zeros(total.shape[:1] + lane.shape[1:], BF)
    rest = total
    for part in range(3):
        piece = rest.astype(BF)
        rest = rest - piece.astype(F32)
        out = jnp.where(lane == first + part, piece, out)
    return out


def over_tiles(count, tiles, buf, sems, prepare, product, add):
    full = tiles.shape[0] // CHUNK
    last = full * CHUNK
    chunks = jnp.minimum((count + CHUNK - 1) // CHUNK, full)

    def copy(first, size, sem):
        rows = pl.ds(first, size)
        return pltpu.make_async_copy(tiles.at[rows], buf.at[rows], sems.at[sem])

    def chunk(c):
        return copy(c * CHUNK, CHUNK, c)

    def start_chunk(c):
        for part in range(PARTS):
            copy(c * CHUNK + part * (CHUNK // PARTS), CHUNK // PARTS, c).start()

    for c in range(AHEAD):

        @pl.when(c < chunks)
        def _():
            start_chunk(c)

    prepare()

    def run(first, size):
        terms = [product(first + u) for u in range(size)]
        for u in range(size):
            add(first + u, terms[u])

    def step(c, carry):
        @pl.when(c + AHEAD < chunks)
        def _():
            start_chunk(c + AHEAD)

        @pl.when(jnp.logical_and(c + AHEAD == full, count > last))
        def _():
            copy(last, LAST, full).start()

        chunk(c).wait()
        run(c * CHUNK, CHUNK)
        return carry

    lax.fori_loop(0, chunks, step, 0)

    @pl.when(count > last)
    def _():
        copy(last, LAST, full).wait()
        run(last, LAST)


def own_range(row_blocks, lengths, sem):
    copy = pltpu.make_async_copy(row_blocks, lengths, sem)
    copy.start()
    copy.wait()
    own_row = lax.axis_index("row")
    first, length = jnp.int32(0), jnp.int32(0)
    for r in range(row_blocks.shape[0]):
        first = first + jnp.where(r < own_row, lengths[r], 0)
        length = length + jnp.where(r == own_row, lengths[r], 0)
    return first, length


def authority_body(
    index, count, row_blocks, hub, tiles, keep, send, buf, acc, used, lengths, sems, *, from_hbm
):
    live = count[0]
    source = hub
    if from_hbm:
        seeds = pltpu.make_async_copy(hub, used, sems.at[sems.shape[0] - 1])
        seeds.start()
        source = used
    where_from = {}

    def prepare():
        first_block, usable = own_range(row_blocks, lengths, sems.at[sems.shape[0] - 2])
        where_from[0] = first_block
        acc[...] = jnp.zeros_like(acc)
        if from_hbm:
            seeds.wait()
        for s in range(hub.shape[0]):
            block = source[s]
            used[s] = jnp.where(s < usable, block, jnp.zeros_like(block))

    def product(t):
        slot = jnp.clip((index[t] & 0xFFFF) - where_from[0], 0, hub.shape[0] - 1)
        return jnp.dot(used[slot], buf[t], preferred_element_type=F32)

    def add(t, term):
        where = jnp.where(t < live, index[t] >> 16, 128)
        acc[where] = acc[where] + term

    over_tiles(live, tiles, buf, sems, prepare, product, add)
    keep[...] = acc[:64].astype(BF)
    send[...] = acc[64:128].astype(BF)


def hub_body(index, count, row_blocks, *refs):
    *pieces, tiles, out, buf, acc, gathered, lengths, sems = refs
    live = count[0]
    where_from = {}
    size = pieces[0].shape[0]
    slots = out.shape[0] - 1

    def prepare():
        where_from[0], _ = own_range(row_blocks, lengths, sems.at[sems.shape[0] - 2])
        acc[...] = jnp.zeros_like(acc)

        def take(b, squares):
            for q, piece in enumerate(pieces):
                block = piece[b]
                gathered[q * size + b] = block
                values = block.astype(F32)
                squares = squares + values * values
            return squares

        squares = lax.fori_loop(0, size, take, jnp.zeros(pieces[0].shape[1:], F32))
        total = jnp.sum(squares, axis=1, keepdims=True)
        lane = lax.broadcasted_iota(jnp.int32, squares.shape, 1)
        out[slots] = split_sum(total, lane, 3 * lax.axis_index("col"))

    def product(t):
        return lax.dot_general(
            buf[t], gathered[index[t] >> 16], (((1,), (1,)), ((), ())), preferred_element_type=F32
        )

    def add(t, term):
        slot = jnp.clip((index[t] & 0xFFFF) - where_from[0], 0, slots - 1)
        slot = jnp.where(t < live, slot, slots)
        acc[slot] = acc[slot] + term

    over_tiles(live, tiles, buf, sems, prepare, product, add)
    for s in range(slots):
        out[s] = acc[s].T.astype(BF)


SMEM = pl.BlockSpec(memory_space=pltpu.SMEM)
VMEM = pl.BlockSpec(memory_space=pltpu.VMEM)
HBM = pl.BlockSpec(memory_space=pltpu.HBM)
PARAMS = pltpu.CompilerParams(vmem_limit_bytes=48 * 2**20)


def authority_terms(lists, hub, tiles, from_hbm):
    count, side_len, _ = tiles.shape
    vectors = hub.shape[1]
    shape = jax.ShapeDtypeStruct((64, vectors, side_len), BF)
    return pl.pallas_call(
        functools.partial(authority_body, from_hbm=from_hbm),
        name="authority_terms",
        in_specs=[SMEM, SMEM, HBM, HBM if from_hbm else VMEM, HBM],
        out_specs=[VMEM, VMEM],
        out_shape=[shape, shape],
        scratch_shapes=[
            pltpu.VMEM(tiles.shape, BF),
            pltpu.VMEM((129, vectors, side_len), F32),
            pltpu.VMEM(hub.shape, BF),
            pltpu.SMEM(lists[2].shape, jnp.int32),
            pltpu.SemaphoreType.DMA((count // CHUNK + 3,)),
        ],
        compiler_params=PARAMS,
        cost_estimate=pl.CostEstimate(
            flops=2 * count * vectors * side_len**2, bytes_accessed=tiles.size * 2, transcendentals=0
        ),
    )(*lists, hub, tiles)


def hub_terms(lists, pieces, tiles, slot_count):
    count, side_len, _ = tiles.shape
    vectors = pieces[0].shape[1]
    return pl.pallas_call(
        hub_body,
        name="hub_terms",
        in_specs=[SMEM, SMEM, HBM] + [VMEM] * len(pieces) + [HBM],
        out_specs=VMEM,
        out_shape=jax.ShapeDtypeStruct((slot_count + 1, vectors, side_len), BF),
        scratch_shapes=[
            pltpu.VMEM(tiles.shape, BF),
            pltpu.VMEM((slot_count + 1, side_len, vectors), F32),
            pltpu.VMEM((128, vectors, side_len), BF),
            pltpu.SMEM(lists[2].shape, jnp.int32),
            pltpu.SemaphoreType.DMA((count // CHUNK + 3,)),
        ],
        compiler_params=PARAMS,
        cost_estimate=pl.CostEstimate(
            flops=2 * count * vectors * side_len**2, bytes_accessed=tiles.size * 2, transcendentals=0
        ),
    )(*lists, *pieces, tiles)


def added(a, b):
    return a.astype(F32) + b.astype(F32)


def reduce_over_plane(keep, send):
    got = swap_core(send)
    both = [added(part, other) for part, other in zip(jnp.split(keep, 4), jnp.split(got, 4))]
    got = {k: shift(both[k].astype(BF), 0, k).astype(F32) for k in FAR_FIRST}
    mine = (both[0] + got[1] + got[2] + got[3]).astype(BF)
    got = {k: shift(mine, 1, k).astype(F32) for k in FAR_FIRST}
    return (mine.astype(F32) + got[2]) + (got[1] + got[3])


def gather_over_ring(mine):
    got = {k: shift(mine, 0, -k) for k in FAR_FIRST}
    half = [mine, got[1], got[2], got[3]]
    return half + [swap_core(piece) for piece in half]


def sum_over_rows(value):
    size = lax.axis_size("row")
    copies = jnp.broadcast_to(value[None], (size, *value.shape))
    return jnp.sum(lax.all_to_all(copies, "row", 0, 0, tiled=True), axis=0)


def norm_scale(squares, host_count):
    return 1.0 / jnp.sqrt(squares / host_count + 1.0)


def local(hub_seeds, tile_blocks, tile_rows, tile_cols, tile_count, row_blocks):
    own_row = lax.axis_index("row")
    slot_count = hub_seeds.shape[0]
    host_count = RB_DEV * row_blocks.shape[0] * tile_blocks.shape[1]
    lengths = pltpu.with_memory_space_constraint(row_blocks, pltpu.HBM)
    lists = (tile_rows + positions(own_row, tile_cols) * 65536, tile_count, lengths)
    hub = pltpu.with_memory_space_constraint(hub_seeds, pltpu.HBM)
    hub_squares = []
    for iteration in range(ITERS):
        keep, send = authority_terms(lists, hub, tile_blocks, iteration == 0)
        ring = reduce_over_plane(keep, send)
        terms = hub_terms(lists, gather_over_ring(ring.astype(BF)), tile_blocks, slot_count)
        terms = added(terms, swap_y(terms, 0)).astype(BF)
        terms = added(terms, swap_y(terms, 1))
        squares = jnp.sum(terms[slot_count], axis=1)
        scale = norm_scale(squares, host_count)
        raw_hub = terms[:slot_count] * scale[None, :, None]
        hub = raw_hub.astype(BF)
        hub_squares.append(jnp.sum(raw_hub * raw_hub, axis=(0, 2)))
    everyone = sum_over_rows(jnp.concatenate(hub_squares))
    vectors = squares.shape[0]
    open_scale = norm_scale(everyone[:vectors], host_count)
    authority_scale = open_scale * norm_scale(open_scale * open_scale * squares, host_count)
    rest = authority_scale / scale
    hub_scale = rest * norm_scale(rest * rest * everyone[vectors:], host_count)
    second = jnp.where((own_row & 1) == 0, (own_row >> 1) & 3, own_row >> 3)
    own = lax.dynamic_slice_in_dim(ring, second * GROUP, GROUP)
    authority = (own * authority_scale[None, :, None]).astype(BF)
    return authority, (raw_hub * hub_scale[None, :, None]).astype(BF)


def solution(mesh):
    both = ("row", "col")
    return jax.shard_map(
        local,
        mesh=mesh,
        in_specs=(P("row"), P(both), P(both), P(both), P(both), P()),
        out_specs=(P(both), P("row")),
        check_vma=False,
    )
```
